64 devices in a mesh: dp: 4 (over x, y), ep: 16 (over z, core).
Axes of the slice: x: 2, y: 2, z: 8, core: 2. Of those that a mesh axis runs over, the one named last changes fastest.
The devices are a block of a 4x4x8 slice.
Arguments:
- tokens: bfloat16 [2048, 2048], P(('dp', 'ep')), parts along dimension 0
- expert_ids: int32 [2048, 8], P(('dp', 'ep')), parts along dimension 0
- gate_weights: float32 [2048, 8], P(('dp', 'ep')), parts along dimension 0
- slot_ids: int32 [2048, 8], P(('dp', 'ep')), parts along dimension 0
- w_gate: bfloat16 [64, 2048, 1024], P('ep')
- w_up: bfloat16 [64, 2048, 1024], P('ep')
- w_down: bfloat16 [64, 1024, 2048], P('ep')
Outputs:
- output: bfloat16 [2048, 2048], P(('dp', 'ep')), parts along dimension 0
There are 4 independent parts. The reference program is written for one: setup_inputs(seed, part) draws one part's arguments, and reference() takes and returns one part's arrays. A program takes and returns all parts, laid end to end along the dimension named above; an argument that names none is the same for every part.
All inputs are finite; a program needn't handle non-finite values.
Results may differ from the reference program's by a relative error of at most 0.00122.
Values are sent between devices in bfloat16 or wider.
A program may use at most 768 MiB of HBM per device.

```python
import jax
import jax.numpy as jnp
from jax import lax

GROUP_DEVS = 16
TOK_DEV = 32
MODEL_DIM = 2048
FFN_DIM = 1024
EXPERTS = 64
TOP_K = 8

TOKENS = TOK_DEV * GROUP_DEVS
LOCAL_EXP = EXPERTS // GROUP_DEVS
CAPACITY = 2 * TOP_K * TOKENS // EXPERTS


def draw_routing(route_key):
    order_key, shuffle_key = jax.random.split(route_key)
    dev_rank = jax.random.permutation(order_key, GROUP_DEVS)
    quarter = GROUP_DEVS // 4
    mean_load = TOP_K * TOK_DEV // LOCAL_EXP
    dev_load = jnp.where(dev_rank < 2 * quarter, mean_load // 2, jnp.where(dev_rank < 3 * quarter, mean_load, 2 * mean_load))
    exp_load = jnp.repeat(dev_load, LOCAL_EXP, total_repeat_length=EXPERTS).astype(jnp.int32)
    exp_end = jnp.cumsum(exp_load).astype(jnp.int32)
    exp_start = exp_end - exp_load
    flat_pos = jnp.arange(TOP_K * TOKENS, dtype=jnp.int32)
    sorted_exp = jnp.searchsorted(exp_end, flat_pos, side='right').astype(jnp.int32)
    sorted_slot = flat_pos - exp_start[sorted_exp]
    listed_exp = sorted_exp.reshape(TOP_K, TOK_DEV, GROUP_DEVS).transpose(2, 1, 0)
    listed_slot = sorted_slot.reshape(TOP_K, TOK_DEV, GROUP_DEVS).transpose(2, 1, 0)
    scores = jax.random.randint(shuffle_key, (GROUP_DEVS, TOK_DEV), 0, TOK_DEV) * TOK_DEV + jnp.arange(TOK_DEV, dtype=jnp.int32)[None, :]
    shuffle_order = jnp.argsort(scores, axis=1)
    routed_exp = jnp.take_along_axis(listed_exp, shuffle_order[:, :, None], axis=1)
    routed_slot = jnp.take_along_axis(listed_slot, shuffle_order[:, :, None], axis=1)
    return routed_exp.reshape(TOKENS, TOP_K), routed_slot.reshape(TOKENS, TOP_K)


def setup_inputs(seed: int = 0, part: int = 0) -> dict:
    shared_key, parts_key = jax.random.split(jax.random.key(seed))
    part_key = jax.random.fold_in(parts_key, part)
    tok_key, gate_key, route_key = jax.random.split(part_key, 3)
    key_gate_w, key_up_w, key_down_w = jax.random.split(shared_key, 3)
    tokens = jax.random.normal(tok_key, (TOKENS, MODEL_DIM), jnp.float32).astype(jnp.bfloat16)
    gate_logits = 0.5 * jax.random.normal(gate_key, (TOKENS, TOP_K), jnp.float32)
    gate_weights = jax.nn.softmax(gate_logits, axis=-1)
    expert_ids, slot_ids = draw_routing(route_key)
    w_gate = (jax.random.normal(key_gate_w, (EXPERTS, MODEL_DIM, FFN_DIM), jnp.float32) * MODEL_DIM ** -0.5).astype(jnp.bfloat16)
    w_up = (jax.random.normal(key_up_w, (EXPERTS, MODEL_DIM, FFN_DIM), jnp.float32) * MODEL_DIM ** -0.5).astype(jnp.bfloat16)
    w_down = (jax.random.normal(key_down_w, (EXPERTS, FFN_DIM, MODEL_DIM), jnp.float32) * FFN_DIM ** -0.5).astype(jnp.bfloat16)
    return {'tokens': tokens, 'expert_ids': expert_ids, 'gate_weights': gate_weights, 'slot_ids': slot_ids, 'w_gate': w_gate, 'w_up': w_up, 'w_down': w_down}


def expert_ffn(operands):
    buffer, w_gate, w_up, w_down = operands
    gate_h = jnp.dot(buffer, w_gate, preferred_element_type=jnp.float32)
    up_h = jnp.dot(buffer, w_up, preferred_element_type=jnp.float32)
    hidden = (jax.nn.silu(gate_h) * up_h).astype(jnp.bfloat16)
    return jnp.dot(hidden, w_down, preferred_element_type=jnp.float32)


def reference(tokens, expert_ids, gate_weights, slot_ids, w_gate, w_up, w_down):
    buffers = jnp.zeros((EXPERTS, CAPACITY, MODEL_DIM), tokens.dtype)
    for choice in range(TOP_K):
        buffers = buffers.at[expert_ids[:, choice], slot_ids[:, choice]].set(tokens)
    exp_out = lax.map(expert_ffn, (buffers, w_gate, w_up, w_down))
    accum = jnp.zeros((TOKENS, MODEL_DIM), jnp.float32)
    for choice in range(TOP_K):
        accum = accum + gate_weights[:, choice][:, None] * exp_out[expert_ids[:, choice], slot_ids[:, choice]]
    return accum.astype(jnp.bfloat16)
```

```python
import functools

import jax
import jax.numpy as jnp
from jax import lax
from jax.experimental import pallas as pl
from jax.experimental.pallas import tpu as pltpu
from jax.sharding import PartitionSpec as P

CORES = 2
PIECES = 4
COLS = 256
DOWN_SLOTS = 6
MESH = pl.DeviceIdType.MESH
F32 = jnp.float32
BF16 = jnp.bfloat16


def moe_kernel(nz, capacity, tok_hbm, ids_ref, slots_ref, gates_ref, wg_hbm, wu_hbm, wd_hbm, out_ref,
               tok_all, meta_all, wg, wu, wd, pick, pick_t, slot_gate, buf, hid, parts,
               acc, die_out, die_in, ring0, ring1, ring2, ring3,
               in_sem, gate_sem, down_sem, ag_send, ag_recv, agm_send, agm_recv, die_send, die_recv,
               diem_send, diem_recv, sum_send, sum_recv, rs_send, rs_recv):
    rows = tok_hbm.shape[0]
    dim = tok_hbm.shape[1]
    n_exp, _, ffn = wg.shape
    n_col = dim // COLS
    half = rows // 2
    far = nz // 2
    side = nz * rows
    me = lax.axis_index('ep')
    z = me // CORES
    core = me % CORES
    right = {'ep': ((z + 1) % nz) * CORES + core}
    left = {'ep': ((z + nz - 1) % nz) * CORES + core}
    partner = {'ep': z * CORES + (1 - core)}
    nbr = (right, left)
    piece = dim // PIECES

    own = pltpu.make_async_copy(tok_hbm, tok_all.at[0], in_sem)
    own.start()

    def gate_copies(e):
        return (pltpu.make_async_copy(wg_hbm.at[e], wg.at[e], gate_sem.at[e, 0]),
                pltpu.make_async_copy(wu_hbm.at[e], wu.at[e], gate_sem.at[e, 1]))

    def down_copy(q):
        cols = pl.ds(pl.multiple_of(q * COLS, COLS), COLS)
        return pltpu.make_async_copy(wd_hbm.at[:, :, cols], wd.at[lax.rem(q, DOWN_SLOTS)], down_sem.at[q])

    for e in range(n_exp):
        for copy in gate_copies(e):
            copy.start(priority=1)
    for q in range(min(DOWN_SLOTS, n_col)):
        down_copy(q).start(priority=1)

    barrier = pltpu.get_barrier_semaphore()
    for dev in (right, left, partner):
        pl.semaphore_signal(barrier, inc=1, device_id=dev, device_id_type=MESH)

    meta_all[0] = jnp.concatenate(
        [ids_ref[...].astype(F32), slots_ref[...].astype(F32), gates_ref[...],
         jnp.zeros(gates_ref.shape, F32)], axis=1)
    pl.semaphore_wait(barrier, 3)
    own.wait()

    def cols_of(p):
        return pl.ds(p * piece, piece)

    def ring_copy(way, hop, p):
        src = (nz - hop + 1) % nz if way == 0 else hop - 1
        dst = nz - hop if way == 0 else hop
        return pltpu.make_async_remote_copy(
            tok_all.at[src, :, cols_of(p)], tok_all.at[dst, :, cols_of(p)],
            ag_send.at[way, hop - 1, p], ag_recv.at[way, hop - 1, p], device_id=nbr[way], device_id_type=MESH)

    def ring_meta(way, hop):
        src = (nz - hop + 1) % nz if way == 0 else hop - 1
        dst = nz - hop if way == 0 else hop
        return pltpu.make_async_remote_copy(
            meta_all.at[src], meta_all.at[dst], agm_send.at[way, hop - 1], agm_recv.at[way, hop - 1],
            device_id=nbr[way], device_id_type=MESH)

    def die_copy(j, p):
        return pltpu.make_async_remote_copy(
            tok_all.at[j, :, cols_of(p)], tok_all.at[nz + j, :, cols_of(p)],
            die_send.at[j, p], die_recv.at[j, p], device_id=partner, device_id_type=MESH)

    def die_meta(j):
        return pltpu.make_async_remote_copy(
            meta_all.at[j], meta_all.at[nz + j], diem_send.at[j], diem_recv.at[j],
            device_id=partner, device_id_type=MESH)

    def on_ring(way, hop, p):
        if hop < far:
            return True
        return hop == far and (p < PIECES // 2) == (way == 0)

    def meta_on_ring(way, hop):
        return hop < far or (hop == far and way == 0)

    for way in range(2):
        ring_meta(way, 1).start()
    for p in range(PIECES):
        for way in range(2):
            if on_ring(way, 1, p):
                ring_copy(way, 1, p).start()
    die_meta(0).start()
    for p in range(PIECES):
        die_copy(0, p).start()

    def take_meta(hop):
        for way in range(2):
            if meta_on_ring(way, hop):
                ring_meta(way, hop).wait_recv()
                if meta_on_ring(way, hop + 1):
                    ring_meta(way, hop + 1).start()
                die_meta(nz - hop if way == 0 else hop).start()

    def take_tokens(hop):
        for p in range(PIECES):
            for way in range(2):
                if on_ring(way, hop, p):
                    ring_copy(way, hop, p).wait_recv()
                    if on_ring(way, hop + 1, p):
                        ring_copy(way, hop + 1, p).start()
                    die_copy(nz - hop if way == 0 else hop, p).start()

    for hop in range(1, far):
        take_meta(hop)
        take_tokens(hop)
    take_meta(far)
    for j in range(nz):
        die_meta(j).wait_recv()

    lane = lax.broadcasted_iota(jnp.int32, (8, 128), 1)
    per = 128 // rows
    groups = CORES * nz // per
    slot_row = lax.broadcasted_iota(jnp.int32, (capacity, 128), 0).astype(F32) + 1.0
    slot_lane = lax.broadcasted_iota(jnp.int32, (128, capacity), 1).astype(F32) + 1.0
    sums = [jnp.zeros((capacity, 1), F32) for _ in range(n_exp)]
    for g in range(groups):
        ids = jnp.zeros((8, 128), F32)
        slots = jnp.zeros((8, 128), F32)
        gates = jnp.zeros((8, 128), F32)
        for i in range(per):
            tile = meta_all[g * per + i]
            here = (lane >= i * rows) & (lane < (i + 1) * rows)
            ids = jnp.where(here, pltpu.roll(tile, (i * rows) % 128, 1), ids)
            slots = jnp.where(here, pltpu.roll(tile, ((i - 1) * rows) % 128, 1), slots)
            gates = jnp.where(here, pltpu.roll(tile, ((i - 2) * rows) % 128, 1), gates)
        slot_rows = []
        for e in range(n_exp):
            mine = ids == (me * n_exp + e).astype(F32)
            slot_e = jnp.sum(jnp.where(mine, slots + 1.0, 0.0), axis=0, keepdims=True)
            gate_e = jnp.sum(jnp.where(mine, gates, 0.0), axis=0, keepdims=True)
            hit = slot_row == slot_e
            pick[e * capacity:(e + 1) * capacity, g * 128:(g + 1) * 128] = jnp.where(hit, 1.0, 0.0).astype(BF16)
            sums[e] = sums[e] + jnp.sum(jnp.where(hit, gate_e, 0.0), axis=1, keepdims=True)
            slot_rows.append(slot_e)
        table = jnp.concatenate(slot_rows + [jnp.zeros((8 - n_exp, 128), F32)], axis=0).T
        for e in range(n_exp):
            pick_t[g * 128:(g + 1) * 128, e * capacity:(e + 1) * capacity] = jnp.where(
                slot_lane == table[:, e:e + 1], 1.0, 0.0).astype(BF16)
    for e in range(n_exp):
        slot_gate[e * capacity:(e + 1) * capacity, :] = jnp.broadcast_to(sums[e], (capacity, 128))

    take_tokens(far)
    for j in range(nz):
        for p in range(PIECES):
            die_copy(j, p).wait_recv()

    tok_rows = tok_all.shape[0] * rows

    @pl.loop(0, dim // 512)
    def _(n):
        cols = pl.ds(pl.multiple_of(n * 512, 512), 512)
        block = tok_all[:, :, cols].reshape(tok_rows, 512)
        buf[:, cols] = jnp.dot(pick[...], block, preferred_element_type=F32).astype(BF16)

    @pl.loop(0, n_exp)
    def _(e):
        for copy in gate_copies(e):
            copy.wait()
        here = pl.ds(pl.multiple_of(e * capacity, capacity), capacity)

        @pl.loop(0, ffn // 512)
        def _(n):
            cols = pl.ds(pl.multiple_of(n * 512, 512), 512)
            x = buf[here, :]
            gate_h = jnp.dot(x, wg[e, :, cols], preferred_element_type=F32)
            up_h = jnp.dot(x, wu[e, :, cols], preferred_element_type=F32)
            hid[here, cols] = (jax.nn.silu(gate_h) * up_h).astype(BF16)

    def sum_copy(q):
        return pltpu.make_async_remote_copy(
            die_out.at[lax.rem(q, 2)], die_in.at[q], sum_send.at[lax.rem(q, 2)], sum_recv.at[q],
            device_id=partner, device_id_type=MESH)

    def block_of(way, step):
        return far - step if way == 0 else (far + step) % nz

    def rs_copy(way, kind, q):
        first = slice(0, half) if way == 0 else slice(half, rows)
        second = slice(half, rows) if way == 0 else slice(0, half)
        step, part, dst = ((0, first, ring0), (1, second, ring1), (1, first, ring1),
                           (2, slice(0, rows), ring2), (3, slice(0, rows), ring3))[kind]
        base = block_of(way, step) * rows
        src = acc.at[q, pl.ds(base + part.start, part.stop - part.start), :]
        if kind == 0:
            to = ring0.at[way, q]
        else:
            to = dst.at[way, q, pl.ds(part.start, part.stop - part.start), :]
        return pltpu.make_async_remote_copy(
            src, to, rs_send.at[way, kind, q], rs_recv.at[way, kind, q], device_id=nbr[way], device_id_type=MESH)

    def send_own(q):
        sum_copy(q).wait_recv()
        acc[q] = acc[q] + die_in[q]
        for kind in (0, 1):
            for way in range(2):
                rs_copy(way, kind, q).start()

    @pl.loop(0, n_col)
    def _(q):
        down_copy(q).wait()
        slot = lax.rem(q, DOWN_SLOTS)
        for e in range(n_exp):
            span = slice(e * capacity, (e + 1) * capacity)
            res = jnp.dot(hid[span, :], wd[slot, e], preferred_element_type=F32)
            weights = slot_gate[span, :]
            res = res * jnp.concatenate([weights] * (COLS // 128), axis=1)
            hi = res.astype(BF16)
            rest = res - hi.astype(F32)
            mid = rest.astype(BF16)
            parts[0, span, :] = hi
            parts[1, span, :] = mid
            parts[2, span, :] = (rest - mid.astype(F32)).astype(BF16)

        def added(lo):
            onehot = pick_t[lo:lo + side, :]
            return (jnp.dot(onehot, parts[0], preferred_element_type=F32)
                    + jnp.dot(onehot, parts[1], preferred_element_type=F32)
                    + jnp.dot(onehot, parts[2], preferred_element_type=F32))

        @pl.when(q >= 2)
        def _():
            sum_copy(q - 2).wait_send()

        die_out[lax.rem(q, 2)] = added(side)
        sum_copy(q).start()
        acc[q] = added(0)

        @pl.when(q + DOWN_SLOTS < n_col)
        def _():
            down_copy(q + DOWN_SLOTS).start(priority=1)

        @pl.when(q >= 1)
        def _():
            send_own(q - 1)

    send_own(n_col - 1)

    @pl.loop(0, n_col)
    def _(q):
        for way in range(2):
            rs_copy(way, 0, q).wait_recv()
            lo = block_of(way, 1) * rows + (0 if way == 0 else half)
            acc[q, lo:lo + half, :] = acc[q, lo:lo + half, :] + ring0[way, q]
            rs_copy(way, 2, q).start()

    for step, ring, kinds in ((2, ring1, (1, 2)), (3, ring2, (3,))):
        @pl.loop(0, n_col)
        def _(q):
            for way in range(2):
                for kind in kinds:
                    rs_copy(way, kind, q).wait_recv()
                lo = block_of(way, step) * rows
                acc[q, lo:lo + rows, :] = acc[q, lo:lo + rows, :] + ring[way, q]
                rs_copy(way, step + 1, q).start()

    @pl.loop(0, n_col)
    def _(q):
        for way in range(2):
            rs_copy(way, 4, q).wait_recv()
        cols = pl.ds(pl.multiple_of(q * COLS, COLS), COLS)
        out_ref[:, cols] = (acc[q, 0:rows, :] + (ring3[0, q] + ring3[1, q])).astype(out_ref.dtype)

    for way in range(2):
        for hop in range(1, far + 1):
            if meta_on_ring(way, hop):
                ring_meta(way, hop).wait_send()
            for p in range(PIECES):
                if on_ring(way, hop, p):
                    ring_copy(way, hop, p).wait_send()
    for j in range(nz):
        die_meta(j).wait_send()
        for p in range(PIECES):
            die_copy(j, p).wait_send()
    for q in range(max(n_col - 2, 0), n_col):
        sum_copy(q).wait_send()

    @pl.loop(0, n_col)
    def _(q):
        for way in range(2):
            for kind in range(5):
                rs_copy(way, kind, q).wait_send()


def solution(mesh):
    row_spec = P(('dp', 'ep'), None)
    exp_spec = P('ep', None, None)
    devs = mesh.shape['ep']
    nz = devs // CORES

    def local_moe(tok_rows, expert_ids, gate_weights, slot_ids, w_gate, w_up, w_down):
        rows, dim = tok_rows.shape
        top_k = expert_ids.shape[1]
        n_exp, _, ffn = w_gate.shape
        capacity = 2 * top_k * rows // n_exp
        n_col = dim // COLS
        far = nz // 2
        slots = n_exp * capacity
        total = devs * rows
        dma = pltpu.SemaphoreType.DMA
        vmem = pltpu.VMEM
        scratch = [
            vmem((devs, rows, dim), BF16), vmem((devs, 8, 128), F32),
            vmem((n_exp, dim, ffn), BF16), vmem((n_exp, dim, ffn), BF16),
            vmem((min(DOWN_SLOTS, n_col), n_exp, ffn, COLS), BF16),
            vmem((slots, total), BF16), vmem((total, slots), BF16), vmem((slots, 128), F32),
            vmem((slots, dim), BF16), vmem((slots, ffn), BF16), vmem((3, slots, COLS), BF16),
            vmem((n_col, nz * rows, COLS), F32), vmem((2, nz * rows, COLS), F32), vmem((n_col, nz * rows, COLS), F32),
            vmem((2, n_col, rows // 2, COLS), F32),
            vmem((2, n_col, rows, COLS), F32), vmem((2, n_col, rows, COLS), F32), vmem((2, n_col, rows, COLS), F32),
            dma, dma((n_exp, 2)), dma((n_col,)),
            dma((2, far, PIECES)), dma((2, far, PIECES)), dma((2, far)), dma((2, far)),
            dma((nz, PIECES)), dma((nz, PIECES)), dma((nz,)), dma((nz,)),
            dma((2,)), dma((n_col,)),
            dma((2, 5, n_col)), dma((2, 5, n_col)),
        ]
        anyspace = pl.BlockSpec(memory_space=pl.ANY)
        in_vmem = pl.BlockSpec(memory_space=pltpu.VMEM)
        flops = 6 * slots * dim * ffn
        return pl.pallas_call(
            functools.partial(moe_kernel, nz, capacity),
            out_shape=jax.ShapeDtypeStruct((rows, dim), tok_rows.dtype),
            in_specs=[anyspace, in_vmem, in_vmem, in_vmem, anyspace, anyspace, anyspace],
            out_specs=in_vmem,
            scratch_shapes=scratch,
            name='routed_experts',
            cost_estimate=pl.CostEstimate(flops=flops, bytes_accessed=6 * n_exp * dim * ffn, transcendentals=slots * ffn),
            compiler_params=pltpu.CompilerParams(
                collective_id=0, has_side_effects=True, vmem_limit_bytes=67043328),
        )(tok_rows, expert_ids.T, slot_ids.T, gate_weights.T, w_gate, w_up, w_down)

    return jax.shard_map(local_moe, mesh=mesh, in_specs=(row_spec, row_spec, row_spec, row_spec, exp_spec, exp_spec, exp_spec), out_specs=row_spec, check_vma=False)
```

```python
import functools

import jax
import jax.numpy as jnp
from jax import lax
from jax.experimental import pallas as pl
from jax.experimental.pallas import tpu as pltpu
from jax.sharding import PartitionSpec as P

CORES = 2
PIECES = 4
COLS = 256
DOWN_SLOTS = 6
MESH = pl.DeviceIdType.MESH
F32 = jnp.float32
BF16 = jnp.bfloat16


def moe_kernel(nz, capacity, tok_hbm, ids_hbm, slots_hbm, gates_hbm, wg_hbm, wu_hbm, wd_hbm, out_ref,
               ids_ref, slots_ref, gates_ref, tok_all, meta_all, wg, wu, wd, pick, pick_t, slot_gate, buf, hid, parts_a, parts_b,
               acc, die_out, die_in, ring0, ring1, ring2, ring3,
               in_sem, route_sem, gate_sem, down_sem, ag_send, ag_recv, agm_send, agm_recv, die_send, die_recv,
               diem_send, diem_recv, sum_send, sum_recv, rs_send, rs_recv):
    rows = tok_hbm.shape[0]
    dim = tok_hbm.shape[1]
    n_exp, _, ffn = wg.shape
    n_col = dim // COLS
    half = rows // 2
    far = nz // 2
    side = nz * rows
    me = lax.axis_index('ep')
    z = me // CORES
    core = me % CORES
    right = {'ep': ((z + 1) % nz) * CORES + core}
    left = {'ep': ((z + nz - 1) % nz) * CORES + core}
    partner = {'ep': z * CORES + (1 - core)}
    nbr = (right, left)
    piece = dim // PIECES

    barrier = pltpu.get_barrier_semaphore()
    for dev in (right, left, partner):
        pl.semaphore_signal(barrier, inc=1, device_id=dev, device_id_type=MESH)
    own = pltpu.make_async_copy(tok_hbm, tok_all.at[0], in_sem)
    own.start()
    routes = [pltpu.make_async_copy(src, dst, route_sem.at[i]) for i, (src, dst) in enumerate(
        ((ids_hbm, ids_ref), (slots_hbm, slots_ref), (gates_hbm, gates_ref)))]
    for copy in routes:
        copy.start()

    def gate_copies(e):
        return (pltpu.make_async_copy(wg_hbm.at[e], wg.at[e], gate_sem.at[e, 0]),
                pltpu.make_async_copy(wu_hbm.at[e], wu.at[e], gate_sem.at[e, 1]))

    def down_copy(q):
        cols = pl.ds(pl.multiple_of(q * COLS, COLS), COLS)
        return pltpu.make_async_copy(wd_hbm.at[:, :, cols], wd.at[lax.rem(q, DOWN_SLOTS)], down_sem.at[q])

    for e in range(n_exp):
        for copy in gate_copies(e):
            copy.start(priority=1)
    for q in range(min(DOWN_SLOTS, n_col)):
        down_copy(q).start(priority=1)

    for copy in routes:
        copy.wait()
    meta_all[0] = jnp.concatenate(
        [ids_ref[...].astype(F32), slots_ref[...].astype(F32), gates_ref[...],
         jnp.zeros(gates_ref.shape, F32)], axis=1)
    pl.semaphore_wait(barrier, 3)
    own.wait()

    order = [0]
    for hop in range(1, far):
        order += [hop, nz - hop]
    order.append(far)
    place = {j: order.index(j) for j in range(nz)}
    quad = nz // 2

    def spot(other, j):
        return (place[j] // quad) * nz + other * quad + place[j] % quad

    def cols_of(p):
        return pl.ds(p * piece, piece)

    def ring_copy(way, hop, p):
        src = (nz - hop + 1) % nz if way == 0 else hop - 1
        dst = nz - hop if way == 0 else hop
        return pltpu.make_async_remote_copy(
            tok_all.at[spot(0, src), :, cols_of(p)], tok_all.at[spot(0, dst), :, cols_of(p)],
            ag_send.at[way, hop - 1, p], ag_recv.at[way, hop - 1, p], device_id=nbr[way], device_id_type=MESH)

    def ring_meta(way, hop):
        src = (nz - hop + 1) % nz if way == 0 else hop - 1
        dst = nz - hop if way == 0 else hop
        return pltpu.make_async_remote_copy(
            meta_all.at[spot(0, src)], meta_all.at[spot(0, dst)], agm_send.at[way, hop - 1], agm_recv.at[way, hop - 1],
            device_id=nbr[way], device_id_type=MESH)

    def die_copy(j, p):
        return pltpu.make_async_remote_copy(
            tok_all.at[spot(0, j), :, cols_of(p)], tok_all.at[spot(1, j), :, cols_of(p)],
            die_send.at[j, p], die_recv.at[j, p], device_id=partner, device_id_type=MESH)

    def die_meta(j):
        return pltpu.make_async_remote_copy(
            meta_all.at[spot(0, j)], meta_all.at[spot(1, j)], diem_send.at[j], diem_recv.at[j],
            device_id=partner, device_id_type=MESH)

    def on_ring(way, hop, p):
        if hop < far:
            return True
        return hop == far and (p < PIECES // 2) == (way == 0)

    def meta_on_ring(way, hop):
        return hop < far or (hop == far and way == 0)

    for way in range(2):
        ring_meta(way, 1).start()
    for p in range(PIECES):
        for way in range(2):
            if on_ring(way, 1, p):
                ring_copy(way, 1, p).start()
    die_meta(0).start()
    for p in range(PIECES):
        die_copy(0, p).start()

    def take_meta(hop):
        for way in range(2):
            if meta_on_ring(way, hop):
                ring_meta(way, hop).wait_recv()
                if meta_on_ring(way, hop + 1):
                    ring_meta(way, hop + 1).start()
                die_meta(nz - hop if way == 0 else hop).start()

    def take_tokens(hop):
        for p in range(PIECES):
            for way in range(2):
                if on_ring(way, hop, p):
                    ring_copy(way, hop, p).wait_recv()
                    if on_ring(way, hop + 1, p):
                        ring_copy(way, hop + 1, p).start()
                    die_copy(nz - hop if way == 0 else hop, p).start()

    lane = lax.broadcasted_iota(jnp.int32, (8, 128), 1)
    per = 128 // rows
    slot_row = lax.broadcasted_iota(jnp.int32, (capacity, 128), 0).astype(F32) + 1.0
    slot_lane = lax.broadcasted_iota(jnp.int32, (128, capacity), 1).astype(F32) + 1.0

    def one_hots(g):
        ids = jnp.zeros((8, 128), F32)
        slots = jnp.zeros((8, 128), F32)
        gates = jnp.zeros((8, 128), F32)
        for i in range(per):
            tile = meta_all[g * per + i]
            here = (lane >= i * rows) & (lane < (i + 1) * rows)
            ids = jnp.where(here, pltpu.roll(tile, (i * rows) % 128, 1), ids)
            slots = jnp.where(here, pltpu.roll(tile, ((i - 1) * rows) % 128, 1), slots)
            gates = jnp.where(here, pltpu.roll(tile, ((i - 2) * rows) % 128, 1), gates)
        slot_rows = []
        for e in range(n_exp):
            mine = ids == (me * n_exp + e).astype(F32)
            slot_e = jnp.sum(jnp.where(mine, slots + 1.0, 0.0), axis=0, keepdims=True)
            gate_e = jnp.sum(jnp.where(mine, gates, 0.0), axis=0, keepdims=True)
            hit = slot_row == slot_e
            span = slice(e * capacity, (e + 1) * capacity)
            pick[span, g * 128:(g + 1) * 128] = jnp.where(hit, 1.0, 0.0).astype(BF16)
            gate_sum = jnp.broadcast_to(jnp.sum(jnp.where(hit, gate_e, 0.0), axis=1, keepdims=True), (capacity, 128))
            slot_gate[span, :] = gate_sum if g == 0 else slot_gate[span, :] + gate_sum
            slot_rows.append(slot_e)
        table = jnp.concatenate(slot_rows + [jnp.zeros((8 - n_exp, 128), F32)], axis=0).T
        base = ((g % 2) * 2 + g // 2) * 128
        for e in range(n_exp):
            pick_t[base:base + 128, e * capacity:(e + 1) * capacity] = jnp.where(
                slot_lane == table[:, e:e + 1], 1.0, 0.0).astype(BF16)

    def gather(part):
        @pl.loop(0, dim // 512)
        def _(n):
            cols = pl.ds(pl.multiple_of(n * 512, 512), 512)
            block = tok_all[part * nz:(part + 1) * nz, :, cols].reshape(nz * rows, 512)
            got = jnp.dot(pick[:, part * nz * rows:(part + 1) * nz * rows], block, preferred_element_type=F32)
            if part == 0:
                buf[:, cols] = got.astype(BF16)
            else:
                buf[:, cols] = (buf[:, cols].astype(F32) + got).astype(BF16)

    def die_ready(blocks):
        for j in blocks:
            for p in range(PIECES):
                die_copy(j, p).wait_recv()

    for hop in range(1, far):
        take_meta(hop)
        take_tokens(hop)
    for j in order[:quad]:
        die_meta(j).wait_recv()
    one_hots(0)
    one_hots(1)
    die_ready(order[:quad])
    gather(0)
    take_meta(far)
    for j in order[quad:]:
        die_meta(j).wait_recv()
    one_hots(2)
    one_hots(3)
    take_tokens(far)
    die_ready(order[quad:])
    gather(1)

    @pl.loop(0, n_exp)
    def _(e):
        for copy in gate_copies(e):
            copy.wait()
        here = pl.ds(pl.multiple_of(e * capacity, capacity), capacity)
        for n in range(ffn // 512):
            cols = slice(n * 512, (n + 1) * 512)
            x = buf[here, :]
            gate_h = jnp.dot(x, wg[e, :, cols], preferred_element_type=F32)
            up_h = jnp.dot(x, wu[e, :, cols], preferred_element_type=F32)
            hid[here, cols] = (jax.nn.silu(gate_h) * up_h).astype(BF16)

    def sum_copy(q):
        return pltpu.make_async_remote_copy(
            die_out.at[lax.rem(q, 2)], die_in.at[q], sum_send.at[lax.rem(q, 2)], sum_recv.at[q],
            device_id=partner, device_id_type=MESH)

    def block_of(way, step):
        return far - step if way == 0 else (far + step) % nz

    def rs_copy(way, kind, q):
        first = slice(0, half) if way == 0 else slice(half, rows)
        second = slice(half, rows) if way == 0 else slice(0, half)
        step, part, dst = ((0, first, ring0), (1, second, ring1), (1, first, ring1),
                           (2, slice(0, rows), ring2), (3, slice(0, rows), ring3))[kind]
        base = place[block_of(way, step)] * rows
        src = acc.at[q, pl.ds(base + part.start, part.stop - part.start), :]
        if kind == 0:
            to = ring0.at[way, q]
        else:
            to = dst.at[way, q, pl.ds(part.start, part.stop - part.start), :]
        return pltpu.make_async_remote_copy(
            src, to, rs_send.at[way, kind, q], rs_recv.at[way, kind, q], device_id=nbr[way], device_id_type=MESH)

    def send_own(q):
        sum_copy(q).wait_recv()
        acc[q] = acc[q] + die_in[q]
        for kind in (0, 1):
            for way in range(2):
                rs_copy(way, kind, q).start()

    parts = (parts_a, parts_b)

    def project(q):
        into = parts[q % 2]
        for e in range(n_exp):
            span = slice(e * capacity, (e + 1) * capacity)
            res = jnp.dot(hid[span, :], wd[q % DOWN_SLOTS, e], preferred_element_type=F32)
            res = res * jnp.concatenate([slot_gate[span, :]] * (COLS // 128), axis=1)
            hi = res.astype(BF16)
            rest = res - hi.astype(F32)
            mid = rest.astype(BF16)
            into[0, span, :] = hi
            into[1, span, :] = mid
            into[2, span, :] = (rest - mid.astype(F32)).astype(BF16)

    def added(q, lo):
        onehot = pick_t[lo:lo + side, :]
        part = parts[q % 2]
        return (jnp.dot(onehot, part[0], preferred_element_type=F32)
                + jnp.dot(onehot, part[1], preferred_element_type=F32)
                + jnp.dot(onehot, part[2], preferred_element_type=F32))

    down_copy(0).wait()
    project(0)
    for q in range(n_col):
        if q + 1 < n_col:
            down_copy(q + 1).wait()
        if q >= 2:
            sum_copy(q - 2).wait_send()
        die_out[q % 2] = added(q, side)
        acc[q] = added(q, 0)
        if q + 1 < n_col:
            project(q + 1)
        sum_copy(q).start()
        if q + DOWN_SLOTS < n_col:
            down_copy(q + DOWN_SLOTS).start(priority=1)
        if q >= 1:
            send_own(q - 1)

    send_own(n_col - 1)

    @pl.loop(0, n_col)
    def _(q):
        for way in range(2):
            rs_copy(way, 0, q).wait_recv()
            lo = place[block_of(way, 1)] * rows + (0 if way == 0 else half)
            acc[q, lo:lo + half, :] = acc[q, lo:lo + half, :] + ring0[way, q]
            rs_copy(way, 2, q).start()

    for step, ring, kinds in ((2, ring1, (1, 2)), (3, ring2, (3,))):
        @pl.loop(0, n_col)
        def _(q):
            for way in range(2):
                for kind in kinds:
                    rs_copy(way, kind, q).wait_recv()
                lo = place[block_of(way, step)] * rows
                acc[q, lo:lo + rows, :] = acc[q, lo:lo + rows, :] + ring[way, q]
                rs_copy(way, step + 1, q).start()

    @pl.loop(0, n_col)
    def _(q):
        for way in range(2):
            rs_copy(way, 4, q).wait_recv()
        cols = pl.ds(pl.multiple_of(q * COLS, COLS), COLS)
        out_ref[:, cols] = (acc[q, 0:rows, :] + (ring3[0, q] + ring3[1, q])).astype(out_ref.dtype)

    for way in range(2):
        for hop in range(1, far + 1):
            if meta_on_ring(way, hop):
                ring_meta(way, hop).wait_send()
            for p in range(PIECES):
                if on_ring(way, hop, p):
                    ring_copy(way, hop, p).wait_send()
    for j in range(nz):
        die_meta(j).wait_send()
        for p in range(PIECES):
            die_copy(j, p).wait_send()
    for q in range(max(n_col - 2, 0), n_col):
        sum_copy(q).wait_send()

    @pl.loop(0, n_col)
    def _(q):
        for way in range(2):
            for kind in range(5):
                rs_copy(way, kind, q).wait_send()


def solution(mesh):
    row_spec = P(('dp', 'ep'), None)
    exp_spec = P('ep', None, None)
    devs = mesh.shape['ep']
    nz = devs // CORES

    def local_moe(tok_rows, expert_ids, gate_weights, slot_ids, w_gate, w_up, w_down):
        rows, dim = tok_rows.shape
        top_k = expert_ids.shape[1]
        n_exp, _, ffn = w_gate.shape
        capacity = 2 * top_k * rows // n_exp
        n_col = dim // COLS
        far = nz // 2
        slots = n_exp * capacity
        total = devs * rows
        dma = pltpu.SemaphoreType.DMA
        vmem = pltpu.VMEM
        scratch = [
            vmem((top_k, rows), jnp.int32), vmem((top_k, rows), jnp.int32), vmem((top_k, rows), F32),
            vmem((devs, rows, dim), BF16), vmem((devs, 8, 128), F32),
            vmem((n_exp, dim, ffn), BF16), vmem((n_exp, dim, ffn), BF16),
            vmem((min(DOWN_SLOTS, n_col), n_exp, ffn, COLS), BF16),
            vmem((slots, total), BF16), vmem((total, slots), BF16), vmem((slots, 128), F32),
            vmem((slots, dim), BF16), vmem((slots, ffn), BF16), vmem((3, slots, COLS), BF16), vmem((3, slots, COLS), BF16),
            vmem((n_col, nz * rows, COLS), F32), vmem((2, nz * rows, COLS), F32), vmem((n_col, nz * rows, COLS), F32),
            vmem((2, n_col, rows // 2, COLS), F32),
            vmem((2, n_col, rows, COLS), F32), vmem((2, n_col, rows, COLS), F32), vmem((2, n_col, rows, COLS), F32),
            dma, dma((3,)), dma((n_exp, 2)), dma((n_col,)),
            dma((2, far, PIECES)), dma((2, far, PIECES)), dma((2, far)), dma((2, far)),
            dma((nz, PIECES)), dma((nz, PIECES)), dma((nz,)), dma((nz,)),
            dma((2,)), dma((n_col,)),
            dma((2, 5, n_col)), dma((2, 5, n_col)),
        ]
        anyspace = pl.BlockSpec(memory_space=pl.ANY)
        in_vmem = pl.BlockSpec(memory_space=pltpu.VMEM)
        flops = 6 * slots * dim * ffn
        return pl.pallas_call(
            functools.partial(moe_kernel, nz, capacity),
            out_shape=jax.ShapeDtypeStruct((rows, dim), tok_rows.dtype),
            in_specs=[anyspace] * 7,
            out_specs=in_vmem,
            scratch_shapes=scratch,
            name='routed_experts',
            cost_estimate=pl.CostEstimate(flops=flops, bytes_accessed=6 * n_exp * dim * ffn, transcendentals=slots * ffn),
            compiler_params=pltpu.CompilerParams(
                collective_id=0, has_side_effects=True, vmem_limit_bytes=67043328),
        )(tok_rows, expert_ids.T, slot_ids.T, gate_weights.T, w_gate, w_up, w_down)

    return jax.shard_map(local_moe, mesh=mesh, in_specs=(row_spec, row_spec, row_spec, row_spec, exp_spec, exp_spec, exp_spec), out_specs=row_spec, check_vma=False)
```

```python
import functools

import jax
import jax.numpy as jnp
from jax import lax
from jax.experimental import pallas as pl
from jax.experimental.pallas import tpu as pltpu
from jax.sharding import PartitionSpec as P

CORES = 2
HALVES = 2
PIECES = 2
COLS = 512
MESH = pl.DeviceIdType.MESH
F32 = jnp.float32
BF16 = jnp.bfloat16


def moe_kernel(nz, capacity, tok_hbm, ids_hbm, slots_hbm, gates_hbm, wg_hbm, wu_hbm, wd_hbm, out_ref,
               ids_ref, slots_ref, gates_ref, tok, meta_all, wg, wu, wd, pick, pick_t, slot_gate, buf, hid,
               parts_a, parts_b, acc, die_out, die_in, ring0, ring1, ring2, ring3,
               in_sem, route_sem, gate_sem, down_sem, ag_send, ag_recv, agm_send, agm_recv, die_send, die_recv,
               diem_send, diem_recv, sum_send, sum_recv, rs_send, rs_recv):
    rows, dim = tok_hbm.shape
    n_exp, _, ffn = wg.shape
    n_col = dim // COLS
    hr = rows // HALVES
    far = nz // 2
    side = nz * hr
    me = lax.axis_index('ep')
    z = me // CORES
    core = me % CORES
    right = {'ep': ((z + 1) % nz) * CORES + core}
    left = {'ep': ((z + nz - 1) % nz) * CORES + core}
    partner = {'ep': z * CORES + (1 - core)}
    nbr = (right, left)
    piece = dim // PIECES

    barrier = pltpu.get_barrier_semaphore()
    for dev in (right, left, partner):
        pl.semaphore_signal(barrier, inc=1, device_id=dev, device_id_type=MESH)

    def own_copy(h):
        return pltpu.make_async_copy(tok_hbm.at[h * hr:(h + 1) * hr], tok.at[h, 0], in_sem.at[h])

    routes = [pltpu.make_async_copy(src, dst, route_sem.at[i]) for i, (src, dst) in enumerate(
        ((ids_hbm, ids_ref), (slots_hbm, slots_ref), (gates_hbm, gates_ref)))]
    for copy in routes:
        copy.start()
    for h in range(HALVES):
        own_copy(h).start()

    def gate_copies(e):
        return (pltpu.make_async_copy(wg_hbm.at[e], wg.at[e], gate_sem.at[e, 0]),
                pltpu.make_async_copy(wu_hbm.at[e], wu.at[e], gate_sem.at[e, 1]))

    def down_copy(q):
        return pltpu.make_async_copy(wd_hbm.at[:, :, q * COLS:(q + 1) * COLS], wd.at[q], down_sem.at[q])

    for e in range(n_exp):
        for copy in gate_copies(e):
            copy.start(priority=1)
    for q in range(n_col):
        down_copy(q).start(priority=1)

    for copy in routes:
        copy.wait()
    meta_all[0] = jnp.concatenate(
        [ids_ref[...].astype(F32), slots_ref[...].astype(F32), gates_ref[...],
         jnp.zeros(gates_ref.shape, F32)], axis=1)
    for h in range(HALVES):
        own_copy(h).wait()
    pl.semaphore_wait(barrier, 3)

    def ends(way, hop):
        return ((nz - hop + 1) % nz, nz - hop) if way == 0 else (hop - 1, hop)

    def ring_copy(h, way, hop, p):
        src, dst = ends(way, hop)
        cols = pl.ds(p * piece, piece)
        return pltpu.make_async_remote_copy(
            tok.at[h, src, :, cols], tok.at[h, dst, :, cols],
            ag_send.at[h, way, hop - 1, p], ag_recv.at[h, way, hop - 1, p], device_id=nbr[way], device_id_type=MESH)

    def ring_meta(way, hop):
        src, dst = ends(way, hop)
        return pltpu.make_async_remote_copy(
            meta_all.at[src], meta_all.at[dst], agm_send.at[way, hop - 1], agm_recv.at[way, hop - 1],
            device_id=nbr[way], device_id_type=MESH)

    def die_copy(h, j, p):
        cols = pl.ds(p * piece, piece)
        return pltpu.make_async_remote_copy(
            tok.at[h, j, :, cols], tok.at[h, nz + j, :, cols],
            die_send.at[h, j, p], die_recv.at[h, j, p], device_id=partner, device_id_type=MESH)

    def die_meta(j):
        return pltpu.make_async_remote_copy(
            meta_all.at[j], meta_all.at[nz + j], diem_send.at[j], diem_recv.at[j],
            device_id=partner, device_id_type=MESH)

    def on_ring(way, hop, p):
        return hop < far or (hop == far and (p < PIECES // 2) == (way == 0))

    def meta_on_ring(way, hop):
        return hop < far or (hop == far and way == 0)

    def take_meta(hop):
        for way in range(2):
            if meta_on_ring(way, hop):
                ring_meta(way, hop).wait_recv()
                if meta_on_ring(way, hop + 1):
                    ring_meta(way, hop + 1).start()
                die_meta(ends(way, hop)[1]).start()

    def send_own_block(h, p):
        for way in range(2):
            ring_copy(h, way, 1, p).start()
        die_copy(h, 0, p).start()

    def take_block(h, hop, p):
        for way in range(2):
            if on_ring(way, hop, p):
                ring_copy(h, way, hop, p).wait_recv()
                if on_ring(way, hop + 1, p):
                    ring_copy(h, way, hop + 1, p).start()
                die_copy(h, ends(way, hop)[1], p).start()

    def take_blocks(h, hop):
        for p in range(PIECES):
            take_block(h, hop, p)

    def die_ready(h):
        for j in range(nz):
            for p in range(PIECES):
                die_copy(h, j, p).wait_recv()

    lane = lax.broadcasted_iota(jnp.int32, (8, 128), 1)
    slot_row = lax.broadcasted_iota(jnp.int32, (capacity, 128), 0).astype(F32) + 1.0
    slot_lane = lax.broadcasted_iota(jnp.int32, (128, capacity), 1).astype(F32) + 1.0

    def one_hots(h, other, picks, sums_too):
        ids = jnp.zeros((8, 128), F32)
        slots = jnp.zeros((8, 128), F32)
        gates = jnp.zeros((8, 128), F32)
        for j in range(nz):
            tile = meta_all[other * nz + j]
            here = (lane >= j * hr) & (lane < (j + 1) * hr)
            shift = (j - h) * hr
            ids = jnp.where(here, pltpu.roll(tile, shift % 128, 1), ids)
            slots = jnp.where(here, pltpu.roll(tile, (shift - rows) % 128, 1), slots)
            gates = jnp.where(here, pltpu.roll(tile, (shift - 2 * rows) % 128, 1), gates)
        slot_rows = []
        base = other * 128
        for e in range(n_exp):
            mine = ids == (me * n_exp + e).astype(F32)
            slot_e = jnp.sum(jnp.where(mine, slots + 1.0, 0.0), axis=0, keepdims=True)
            gate_e = jnp.sum(jnp.where(mine, gates, 0.0), axis=0, keepdims=True)
            hit = slot_row == slot_e
            span = slice(e * capacity, (e + 1) * capacity)
            if picks:
                pick[span, base:base + 128] = jnp.where(hit, 1.0, 0.0).astype(BF16)
            if sums_too:
                gate_sum = jnp.broadcast_to(
                    jnp.sum(jnp.where(hit, gate_e, 0.0), axis=1, keepdims=True), (capacity, 128))
                slot_gate[span, :] = gate_sum if h + other == 0 else slot_gate[span, :] + gate_sum
            slot_rows.append(slot_e)
        if not sums_too:
            return
        table = jnp.concatenate(slot_rows + [jnp.zeros((8 - n_exp, 128), F32)], axis=0).T
        for e in range(n_exp):
            pick_t[h, base:base + 128, e * capacity:(e + 1) * capacity] = jnp.where(
                slot_lane == table[:, e:e + 1], 1.0, 0.0).astype(BF16)

    def gather(h):
        for n in range(dim // 512):
            cols = slice(n * 512, (n + 1) * 512)
            block = tok[h, :, :, cols].reshape(CORES * side, 512)
            buf[:, cols] = jnp.dot(pick[...], block, preferred_element_type=F32).astype(BF16)

    def gate_up(e, n):
        span = slice(e * capacity, (e + 1) * capacity)
        cols = slice(n * 512, (n + 1) * 512)
        x = buf[span, :]
        gate_h = jnp.dot(x, wg[e, :, cols], preferred_element_type=F32)
        up_h = jnp.dot(x, wu[e, :, cols], preferred_element_type=F32)
        hid[span, cols] = (jax.nn.silu(gate_h) * up_h).astype(BF16)

    parts = (parts_a, parts_b)

    def project(h, q):
        into = parts[q % 2]
        for e in range(n_exp):
            span = slice(e * capacity, (e + 1) * capacity)
            res = jnp.dot(hid[span, :], wd[q, e], preferred_element_type=F32)
            res = res * jnp.concatenate([slot_gate[span, :]] * (COLS // 128), axis=1)
            hi = res.astype(BF16)
            rest = res - hi.astype(F32)
            mid = rest.astype(BF16)
            into[0, span, :] = hi
            into[1, span, :] = mid
            into[2, span, :] = (rest - mid.astype(F32)).astype(BF16)

    def added(h, q, other):
        onehot = pick_t[h, other * side:(other + 1) * side, :]
        part = parts[q % 2]
        return (jnp.dot(onehot, part[0], preferred_element_type=F32)
                + jnp.dot(onehot, part[1], preferred_element_type=F32)
                + jnp.dot(onehot, part[2], preferred_element_type=F32))

    def sum_copy(h, q):
        return pltpu.make_async_remote_copy(
            die_out.at[q % 2], die_in.at[h, q], sum_send.at[h, q], sum_recv.at[h, q],
            device_id=partner, device_id_type=MESH)

    def block_of(way, step):
        return far - step if way == 0 else (far + step) % nz

    def rows_of(way, step, kind):
        base = block_of(way, step) * hr
        if kind == 'all':
            return base, hr
        return base + (hr // 2 if (kind == 'first') == (way == 1) else 0), hr // 2

    def rs_copy(h, way, kind, q):
        step, part, dst = ((0, 'first', ring0), (1, 'second', ring1), (1, 'first', ring1),
                           (2, 'all', ring2), (3, 'all', ring3))[kind]
        lo, size = rows_of(way, step, part)
        src = acc.at[h, q, pl.ds(lo, size), :]
        to = dst.at[h, way, q, pl.ds(0 if kind == 0 else lo - block_of(way, step) * hr, size), :]
        return pltpu.make_async_remote_copy(
            src, to, rs_send.at[h, way, kind, q], rs_recv.at[h, way, kind, q], device_id=nbr[way], device_id_type=MESH)

    def own_sums(h, q):
        sum_copy(h, q).wait_recv()
        acc[h, q] = acc[h, q] + die_in[h, q]
        for kind in (0, 1):
            for way in range(2):
                rs_copy(h, way, kind, q).start()

    def sums(h, q, step):
        ring, part, kinds = ((ring0, 'first', (0,)), (ring1, 'all', (1, 2)), (ring2, 'all', (3,)))[step - 1]
        for way in range(2):
            for kind in kinds:
                rs_copy(h, way, kind, q).wait_recv()
            lo, size = rows_of(way, step, part)
            acc[h, q, lo:lo + size, :] = acc[h, q, lo:lo + size, :] + ring[h, way, q]
            rs_copy(h, way, step + 1, q).start()

    def finish(h, q):
        for way in range(2):
            rs_copy(h, way, 4, q).wait_recv()
        out_ref[h * hr:(h + 1) * hr, q * COLS:(q + 1) * COLS] = (
            acc[h, q, 0:hr, :] + (ring3[h, 0, q] + ring3[h, 1, q])).astype(out_ref.dtype)

    def experts(h, between):
        for e in range(n_exp):
            if h == 0:
                for copy in gate_copies(e):
                    copy.wait()
            for n in range(ffn // 512):
                gate_up(e, n)
                between(e * (ffn // 512) + n)

    def results(h, between):
        if h == 0:
            down_copy(0).wait()
        project(h, 0)
        for q in range(n_col):
            if h == 0 and q + 1 < n_col:
                down_copy(q + 1).wait()
            if q >= 2:
                sum_copy(h, q - 2).wait_send()
            elif h > 0:
                sum_copy(h - 1, n_col - 2 + q).wait_send()
            die_out[q % 2] = added(h, q, 1)
            acc[h, q] = added(h, q, 0)
            if q + 1 < n_col:
                project(h, q + 1)
            sum_copy(h, q).start()
            between(q)

    a, b = 0, 1
    for way in range(2):
        ring_meta(way, 1).start()
    die_meta(0).start()
    for p in range(PIECES):
        send_own_block(a, p)
    send_own_block(b, 0)
    take_meta(1)
    take_blocks(a, 1)
    send_own_block(b, 1)
    take_meta(2)
    take_blocks(a, 2)
    take_block(b, 1, 0)
    take_meta(3)
    take_blocks(a, 3)
    take_block(b, 1, 1)
    take_meta(4)
    for j in range(nz):
        die_meta(j).wait_recv()
    for h in range(HALVES):
        for other in range(CORES):
            one_hots(h, other, h == a, True)
    take_blocks(a, 4)
    take_block(b, 2, 0)
    die_ready(a)
    gather(a)
    for other in range(CORES):
        one_hots(b, other, True, False)
    take_block(b, 2, 1)

    def after_a(k):
        if k == 0:
            take_block(b, 3, 0)
        if k == 2:
            take_block(b, 3, 1)
        if k == 5:
            take_blocks(b, 4)

    experts(a, after_a)

    def after_ra(q):
        if q >= 1:
            own_sums(a, q - 1)

    results(a, after_ra)
    sums(a, 0, 1)
    die_ready(b)
    gather(b)

    plan = {0: [('own', 3), (1, 1)], 1: [(2, 0)], 2: [(1, 2)], 3: [(2, 1)], 4: [(1, 3), (3, 0)], 5: [(2, 2)],
            6: [(3, 1)], 7: [(2, 3)]}

    def after_b(k):
        for step, q in plan.get(k, ()):
            if step == 'own':
                own_sums(a, q)
            else:
                sums(a, q, step)

    experts(b, after_b)

    def after_rb(q):
        if q == 0:
            sums(a, 2, 3)
            finish(a, 0)
        if q == 1:
            own_sums(b, 0)
            sums(a, 3, 3)
            finish(a, 1)
        if q == 2:
            own_sums(b, 1)
            finish(a, 2)
        if q == 3:
            own_sums(b, 2)
            finish(a, 3)

    results(b, after_rb)
    sums(b, 0, 1)
    own_sums(b, 3)
    for q in range(1, n_col):
        sums(b, q, 1)
    for step in (2, 3):
        for q in range(n_col):
            sums(b, q, step)
    for q in range(n_col):
        finish(b, q)

    for way in range(2):
        for hop in range(1, far + 1):
            if meta_on_ring(way, hop):
                ring_meta(way, hop).wait_send()
            for p in range(PIECES):
                if on_ring(way, hop, p):
                    for h in range(HALVES):
                        ring_copy(h, way, hop, p).wait_send()
    for j in range(nz):
        die_meta(j).wait_send()
        for p in range(PIECES):
            for h in range(HALVES):
                die_copy(h, j, p).wait_send()
    for q in range(n_col - 2, n_col):
        sum_copy(b, q).wait_send()
    for h in range(HALVES):
        for way in range(2):
            for kind in range(5):
                for q in range(n_col):
                    rs_copy(h, way, kind, q).wait_send()


def solution(mesh):
    row_spec = P(('dp', 'ep'), None)
    exp_spec = P('ep', None, None)
    devs = mesh.shape['ep']
    nz = devs // CORES

    def local_moe(tok_rows, expert_ids, gate_weights, slot_ids, w_gate, w_up, w_down):
        rows, dim = tok_rows.shape
        top_k = expert_ids.shape[1]
        n_exp, _, ffn = w_gate.shape
        capacity = 2 * top_k * rows // n_exp
        n_col = dim // COLS
        far = nz // 2
        hr = rows // HALVES
        slots = n_exp * capacity
        half_tok = devs * hr
        dma = pltpu.SemaphoreType.DMA
        vmem = pltpu.VMEM
        scratch = [
            vmem((top_k, rows), jnp.int32), vmem((top_k, rows), jnp.int32), vmem((top_k, rows), F32),
            vmem((HALVES, devs, hr, dim), BF16), vmem((devs, 8, 128), F32),
            vmem((n_exp, dim, ffn), BF16), vmem((n_exp, dim, ffn), BF16), vmem((n_col, n_exp, ffn, COLS), BF16),
            vmem((slots, half_tok), BF16), vmem((HALVES, half_tok, slots), BF16), vmem((slots, 128), F32),
            vmem((slots, dim), BF16), vmem((slots, ffn), BF16), vmem((3, slots, COLS), BF16), vmem((3, slots, COLS), BF16),
            vmem((HALVES, n_col, nz * hr, COLS), F32), vmem((2, nz * hr, COLS), F32), vmem((HALVES, n_col, nz * hr, COLS), F32),
            vmem((HALVES, 2, n_col, hr // 2, COLS), F32), vmem((HALVES, 2, n_col, hr, COLS), F32),
            vmem((HALVES, 2, n_col, hr, COLS), F32), vmem((HALVES, 2, n_col, hr, COLS), F32),
            dma((HALVES,)), dma((3,)), dma((n_exp, 2)), dma((n_col,)),
            dma((HALVES, 2, far, PIECES)), dma((HALVES, 2, far, PIECES)), dma((2, far)), dma((2, far)),
            dma((HALVES, nz, PIECES)), dma((HALVES, nz, PIECES)), dma((nz,)), dma((nz,)),
            dma((HALVES, n_col)), dma((HALVES, n_col)),
            dma((HALVES, 2, 5, n_col)), dma((HALVES, 2, 5, n_col)),
        ]
        anyspace = pl.BlockSpec(memory_space=pl.ANY)
        flops = 6 * slots * dim * ffn
        return pl.pallas_call(
            functools.partial(moe_kernel, nz, capacity),
            out_shape=jax.ShapeDtypeStruct((rows, dim), tok_rows.dtype),
            in_specs=[anyspace] * 7,
            out_specs=pl.BlockSpec(memory_space=pltpu.VMEM),
            scratch_shapes=scratch,
            name='routed_experts',
            cost_estimate=pl.CostEstimate(flops=flops, bytes_accessed=6 * n_exp * dim * ffn, transcendentals=slots * ffn),
            compiler_params=pltpu.CompilerParams(
                collective_id=0, has_side_effects=True, vmem_limit_bytes=67043328),
        )(tok_rows, expert_ids.T, slot_ids.T, gate_weights.T, w_gate, w_up, w_down)

    return jax.shard_map(local_moe, mesh=mesh, in_specs=(row_spec, row_spec, row_spec, row_spec, exp_spec, exp_spec, exp_spec), out_specs=row_spec, check_vma=False)
```

```python
import functools

import jax
import jax.numpy as jnp
from jax import lax
from jax.experimental import pallas as pl
from jax.experimental.pallas import tpu as pltpu
from jax.sharding import PartitionSpec as P

CORES = 2
PIECES = 4
COLS = 512
DOWN_SLOTS = 3
LAGS = (3, 99)
MESH = pl.DeviceIdType.MESH
F32 = jnp.float32
BF16 = jnp.bfloat16


def moe_kernel(nz, capacity, tok_hbm, ids_hbm, slots_hbm, gates_hbm, wg_hbm, wu_hbm, wd_hbm, out_ref,
               ids_ref, slots_ref, gates_ref, tok_all, meta_all, wg, wu, wd, pick, pick_t, slot_gate, buf, hid, parts_a, parts_b,
               acc, die_out, die_in, ring0, ring1, ring2, ring3,
               in_sem, route_sem, gate_sem, down_sem, ag_send, ag_recv, agm_send, agm_recv, die_send, die_recv,
               diem_send, diem_recv, sum_send, sum_recv, rs_send, rs_recv):
    rows = tok_hbm.shape[0]
    dim = tok_hbm.shape[1]
    n_exp, _, ffn = wg.shape
    n_col = dim // COLS
    half = rows // 2
    far = nz // 2
    side = nz * rows
    me = lax.axis_index('ep')
    z = me // CORES
    core = me % CORES
    right = {'ep': ((z + 1) % nz) * CORES + core}
    left = {'ep': ((z + nz - 1) % nz) * CORES + core}
    partner = {'ep': z * CORES + (1 - core)}
    nbr = (right, left)
    piece = dim // PIECES

    barrier = pltpu.get_barrier_semaphore()
    for dev in (right, left, partner):
        pl.semaphore_signal(barrier, inc=1, device_id=dev, device_id_type=MESH)
    own = pltpu.make_async_copy(tok_hbm, tok_all.at[0], in_sem)
    own.start()
    routes = [pltpu.make_async_copy(src, dst, route_sem.at[i]) for i, (src, dst) in enumerate(
        ((ids_hbm, ids_ref), (slots_hbm, slots_ref), (gates_hbm, gates_ref)))]
    for copy in routes:
        copy.start()

    def gate_copies(e):
        return (pltpu.make_async_copy(wg_hbm.at[e], wg.at[e], gate_sem.at[0]),
                pltpu.make_async_copy(wu_hbm.at[e], wu.at[e], gate_sem.at[1]))

    def down_copy(q):
        cols = pl.ds(pl.multiple_of(q * COLS, COLS), COLS)
        return pltpu.make_async_copy(wd_hbm.at[:, :, cols], wd.at[lax.rem(q, DOWN_SLOTS)], down_sem.at[q])

    for e in range(n_exp):
        for copy in gate_copies(e):
            copy.start(priority=1)
    for q in range(min(DOWN_SLOTS, n_col)):
        down_copy(q).start(priority=1)

    for copy in routes:
        copy.wait()
    meta_all[0] = jnp.concatenate(
        [ids_ref[...].astype(F32), slots_ref[...].astype(F32), gates_ref[...],
         jnp.zeros(gates_ref.shape, F32)], axis=1)
    pl.semaphore_wait(barrier, 3)
    own.wait()

    order = [0]
    for hop in range(1, far):
        order += [hop, nz - hop]
    order.append(far)
    place = {j: order.index(j) for j in range(nz)}
    quad = nz // 2

    def spot(other, j):
        return (place[j] // quad) * nz + other * quad + place[j] % quad

    def landed(ref, sem):
        pltpu.make_async_copy(ref, ref, sem).wait()

    def cols_of(p):
        return pl.ds(p * piece, piece)

    def ring_copy(way, hop, p):
        src = (nz - hop + 1) % nz if way == 0 else hop - 1
        dst = nz - hop if way == 0 else hop
        return pltpu.make_async_remote_copy(
            tok_all.at[spot(0, src), :, cols_of(p)], tok_all.at[spot(0, dst), :, cols_of(p)],
            ag_send, ag_recv.at[way, hop - 1, p], device_id=nbr[way], device_id_type=MESH)

    def ring_meta(way, hop):
        src = (nz - hop + 1) % nz if way == 0 else hop - 1
        dst = nz - hop if way == 0 else hop
        return pltpu.make_async_remote_copy(
            meta_all.at[spot(0, src)], meta_all.at[spot(0, dst)], agm_send, agm_recv.at[way, hop - 1],
            device_id=nbr[way], device_id_type=MESH)

    def die_copy(j, p):
        return pltpu.make_async_remote_copy(
            tok_all.at[spot(0, j), :, cols_of(p)], tok_all.at[spot(1, j), :, cols_of(p)],
            die_send, die_recv.at[place[j] // quad], device_id=partner, device_id_type=MESH)

    def die_meta(j):
        return pltpu.make_async_remote_copy(
            meta_all.at[spot(0, j)], meta_all.at[spot(1, j)], diem_send, diem_recv.at[place[j] // quad],
            device_id=partner, device_id_type=MESH)

    def on_ring(way, hop, p):
        if hop < far:
            return True
        return hop == far and (p < PIECES // 2) == (way == 0)

    def meta_on_ring(way, hop):
        return hop < far or (hop == far and way == 0)

    for way in range(2):
        ring_meta(way, 1).start()
    for p in range(PIECES):
        for way in range(2):
            if on_ring(way, 1, p):
                ring_copy(way, 1, p).start()
    die_meta(0).start()
    for p in range(PIECES):
        die_copy(0, p).start()

    def take_meta(hop):
        for way in range(2):
            if meta_on_ring(way, hop):
                ring_meta(way, hop).wait_recv()
                if meta_on_ring(way, hop + 1):
                    ring_meta(way, hop + 1).start()
                die_meta(nz - hop if way == 0 else hop).start()

    def take_tokens(hop, pieces=range(PIECES), fill=()):
        for p in pieces:
            for work in fill[p:p + 1]:
                work()
            for way in range(2):
                if on_ring(way, hop, p):
                    ring_copy(way, hop, p).wait_recv()
                    if on_ring(way, hop + 1, p):
                        ring_copy(way, hop + 1, p).start()
                    die_copy(nz - hop if way == 0 else hop, p).start()

    lane = lax.broadcasted_iota(jnp.int32, (8, 128), 1)
    per = 128 // rows
    slot_row = lax.broadcasted_iota(jnp.int32, (capacity, 128), 0).astype(F32) + 1.0
    slot_lane = lax.broadcasted_iota(jnp.int32, (128, capacity), 1).astype(F32) + 1.0

    def one_hots(g):
        ids = jnp.zeros((8, 128), F32)
        slots = jnp.zeros((8, 128), F32)
        gates = jnp.zeros((8, 128), F32)
        for i in range(per):
            tile = meta_all[g * per + i]
            here = (lane >= i * rows) & (lane < (i + 1) * rows)
            ids = jnp.where(here, pltpu.roll(tile, (i * rows) % 128, 1), ids)
            slots = jnp.where(here, pltpu.roll(tile, ((i - 1) * rows) % 128, 1), slots)
            gates = jnp.where(here, pltpu.roll(tile, ((i - 2) * rows) % 128, 1), gates)
        slot_rows = []
        for e in range(n_exp):
            mine = ids == (me * n_exp + e).astype(F32)
            slot_e = jnp.sum(jnp.where(mine, slots + 1.0, 0.0), axis=0, keepdims=True)
            gate_e = jnp.sum(jnp.where(mine, gates, 0.0), axis=0, keepdims=True)
            hit = slot_row == slot_e
            span = slice(e * capacity, (e + 1) * capacity)
            pick[span, g * 128:(g + 1) * 128] = jnp.where(hit, 1.0, 0.0).astype(BF16)
            gate_sum = jnp.broadcast_to(jnp.sum(jnp.where(hit, gate_e, 0.0), axis=1, keepdims=True), (capacity, 128))
            slot_gate[span, :] = gate_sum if g == 0 else slot_gate[span, :] + gate_sum
            slot_rows.append(slot_e)
        table = jnp.concatenate(slot_rows + [jnp.zeros((8 - n_exp, 128), F32)], axis=0).T
        base = ((g % 2) * 2 + g // 2) * 128
        for e in range(n_exp):
            pick_t[base:base + 128, e * capacity:(e + 1) * capacity] = jnp.where(
                slot_lane == table[:, e:e + 1], 1.0, 0.0).astype(BF16)

    def gather(part, blocks):
        for n in blocks:
            cols = slice(n * 512, (n + 1) * 512)
            block = tok_all[part * nz:(part + 1) * nz, :, cols].reshape(nz * rows, 512)
            got = jnp.dot(pick[:, part * nz * rows:(part + 1) * nz * rows], block, preferred_element_type=F32)
            if part == 0:
                buf[:, cols] = got.astype(BF16)
            else:
                buf[:, cols] = (buf[:, cols].astype(F32) + got).astype(BF16)

    def others(part):
        return slice(part * nz + quad, (part + 1) * nz)

    def near_routes():
        landed(meta_all.at[others(0)], diem_recv.at[0])

    def near_blocks():
        landed(tok_all.at[others(0)], die_recv.at[0])
        gather(0, (0,))

    wide = range(dim // 512)
    fills = {2: [lambda: None, near_routes, lambda: one_hots(0), lambda: one_hots(1)],
             3: [lambda: None, near_blocks] + [functools.partial(gather, 0, (n,)) for n in wide[1:3]]}
    for hop in range(1, far):
        take_meta(hop)
        take_tokens(hop, fill=fills.get(hop, ()))
    take_meta(far)
    gather(0, wide[3:])
    take_tokens(far, range(0, PIECES, 2))
    landed(meta_all.at[others(1)], diem_recv.at[1])
    one_hots(2)
    take_tokens(far, range(1, PIECES, 2))
    one_hots(3)
    landed(tok_all.at[others(1)], die_recv.at[1])
    landed(wg, gate_sem.at[0])
    landed(wu, gate_sem.at[1])
    gather(1, wide)
    for e in range(n_exp):
        here = slice(e * capacity, (e + 1) * capacity)
        for n in range(ffn // 512):
            cols = slice(n * 512, (n + 1) * 512)
            x = buf[here, :]
            gate_h = jnp.dot(x, wg[e, :, cols], preferred_element_type=F32)
            up_h = jnp.dot(x, wu[e, :, cols], preferred_element_type=F32)
            hid[here, cols] = (jax.nn.silu(gate_h) * up_h).astype(BF16)

    def sum_copy(q):
        return pltpu.make_async_remote_copy(
            die_out.at[lax.rem(q, 2)], die_in.at[q], sum_send.at[lax.rem(q, 2)], sum_recv.at[q],
            device_id=partner, device_id_type=MESH)

    def block_of(way, step):
        return far - step if way == 0 else (far + step) % nz

    def rs_copy(way, kind, q):
        first = slice(0, half) if way == 0 else slice(half, rows)
        second = slice(half, rows) if way == 0 else slice(0, half)
        step, part, dst = ((0, first, ring0), (1, second, ring1), (1, first, ring1),
                           (2, slice(0, rows), ring2), (3, slice(0, rows), ring3))[kind]
        base = place[block_of(way, step)] * rows
        src = acc.at[q, pl.ds(base + part.start, part.stop - part.start), :]
        if kind == 0:
            to = ring0.at[way, q]
        else:
            to = dst.at[way, q, pl.ds(part.start, part.stop - part.start), :]
        return pltpu.make_async_remote_copy(
            src, to, rs_send.at[step], rs_recv.at[step, q], device_id=nbr[way], device_id_type=MESH)

    def send_own(q):
        sum_copy(q).wait_recv()
        acc[q] = acc[q] + die_in[q]
        for kind in (0, 1):
            for way in range(2):
                rs_copy(way, kind, q).start()

    rings = (ring0, ring1, ring2, ring3)

    def sums(q, step):
        landed(rings[step - 1].at[:, q], rs_recv.at[step - 1, q])
        for way in range(2):
            lo = place[block_of(way, step)] * rows
            size = rows
            if step == 1:
                lo, size = lo + (0 if way == 0 else half), half
            acc[q, lo:lo + size, :] = acc[q, lo:lo + size, :] + rings[step - 1][way, q]
            rs_copy(way, step + 1, q).start()

    done = {1: 0, 2: 0, 3: 0}
    parts = (parts_a, parts_b)

    def project(q):
        into = parts[q % 2]
        for e in range(n_exp):
            span = slice(e * capacity, (e + 1) * capacity)
            res = jnp.dot(hid[span, :], wd[q % DOWN_SLOTS, e], preferred_element_type=F32)
            res = res * jnp.concatenate([slot_gate[span, :]] * (COLS // 128), axis=1)
            hi = res.astype(BF16)
            rest = res - hi.astype(F32)
            mid = rest.astype(BF16)
            into[0, span, :] = hi
            into[1, span, :] = mid
            into[2, span, :] = (rest - mid.astype(F32)).astype(BF16)

    def added(q, lo):
        onehot = pick_t[lo:lo + side, :]
        part = parts[q % 2]
        return (jnp.dot(onehot, part[0], preferred_element_type=F32)
                + jnp.dot(onehot, part[1], preferred_element_type=F32)
                + jnp.dot(onehot, part[2], preferred_element_type=F32))

    down_copy(0).wait()
    project(0)
    for q in range(n_col):
        if q + 1 < n_col:
            down_copy(q + 1).wait()
        if q >= 2:
            sum_copy(q - 2).wait_send()
        die_out[q % 2] = added(q, side)
        acc[q] = added(q, 0)
        if q + 1 < n_col:
            project(q + 1)
        sum_copy(q).start()
        if q + DOWN_SLOTS < n_col:
            down_copy(q + DOWN_SLOTS).start(priority=1)
        if q >= 1:
            send_own(q - 1)
        for step in (1, 2):
            if q >= LAGS[step - 1]:
                sums(q - LAGS[step - 1], step)
                done[step] = q - LAGS[step - 1] + 1

    send_own(n_col - 1)
    for step in (1, 2, 3):
        for q in range(done[step], n_col):
            sums(q, step)
    for q in range(n_col):
        landed(ring3.at[:, q], rs_recv.at[3, q])
        cols = slice(q * COLS, (q + 1) * COLS)
        out_ref[:, cols] = (acc[q, 0:rows, :] + (ring3[0, q] + ring3[1, q])).astype(out_ref.dtype)

    landed(tok_all.at[0:nz - 1], ag_send)
    landed(tok_all.at[0:nz], die_send)
    landed(meta_all.at[0:nz - 1], agm_send)
    landed(meta_all.at[0:nz], diem_send)
    for q in range(max(n_col - 2, 0), n_col):
        sum_copy(q).wait_send()
    for ring in range(4):
        landed(rings[ring], rs_send.at[ring])


def solution(mesh):
    row_spec = P(('dp', 'ep'), None)
    exp_spec = P('ep', None, None)
    devs = mesh.shape['ep']
    nz = devs // CORES

    def local_moe(tok_rows, expert_ids, gate_weights, slot_ids, w_gate, w_up, w_down):
        rows, dim = tok_rows.shape
        top_k = expert_ids.shape[1]
        n_exp, _, ffn = w_gate.shape
        capacity = 2 * top_k * rows // n_exp
        n_col = dim // COLS
        far = nz // 2
        slots = n_exp * capacity
        total = devs * rows
        dma = pltpu.SemaphoreType.DMA
        vmem = pltpu.VMEM
        scratch = [
            vmem((top_k, rows), jnp.int32), vmem((top_k, rows), jnp.int32), vmem((top_k, rows), F32),
            vmem((devs, rows, dim), BF16), vmem((devs, 8, 128), F32),
            vmem((n_exp, dim, ffn), BF16), vmem((n_exp, dim, ffn), BF16),
            vmem((min(DOWN_SLOTS, n_col), n_exp, ffn, COLS), BF16),
            vmem((slots, total), BF16), vmem((total, slots), BF16), vmem((slots, 128), F32),
            vmem((slots, dim), BF16), vmem((slots, ffn), BF16), vmem((3, slots, COLS), BF16), vmem((3, slots, COLS), BF16),
            vmem((n_col, nz * rows, COLS), F32), vmem((2, nz * rows, COLS), F32), vmem((n_col, nz * rows, COLS), F32),
            vmem((2, n_col, rows // 2, COLS), F32),
            vmem((2, n_col, rows, COLS), F32), vmem((2, n_col, rows, COLS), F32), vmem((2, n_col, rows, COLS), F32),
            dma, dma((3,)), dma((2,)), dma((n_col,)),
            dma, dma((2, far, PIECES)), dma, dma((2, far)),
            dma, dma((2,)), dma, dma((2,)),
            dma((2,)), dma((n_col,)), dma((4,)), dma((4, n_col)),
        ]
        anyspace = pl.BlockSpec(memory_space=pl.ANY)
        in_vmem = pl.BlockSpec(memory_space=pltpu.VMEM)
        flops = 6 * slots * dim * ffn
        return pl.pallas_call(
            functools.partial(moe_kernel, nz, capacity),
            out_shape=jax.ShapeDtypeStruct((rows, dim), tok_rows.dtype),
            in_specs=[anyspace] * 7,
            out_specs=in_vmem,
            scratch_shapes=scratch,
            name='routed_experts',
            cost_estimate=pl.CostEstimate(flops=flops, bytes_accessed=6 * n_exp * dim * ffn, transcendentals=slots * ffn),
            compiler_params=pltpu.CompilerParams(
                collective_id=0, has_side_effects=True, vmem_limit_bytes=67043328),
        )(tok_rows, expert_ids.T, slot_ids.T, gate_weights.T, w_gate, w_up, w_down)

    return jax.shard_map(local_moe, mesh=mesh, in_specs=(row_spec, row_spec, row_spec, row_spec, exp_spec, exp_spec, exp_spec), out_specs=row_spec, check_vma=False)
```

```python
import functools

import jax
import jax.numpy as jnp
from jax import lax
from jax.experimental import pallas as pl
from jax.experimental.pallas import tpu as pltpu
from jax.sharding import PartitionSpec as P

CORES = 2
PIECES = 4
COLS = 512
MESH = pl.DeviceIdType.MESH
F32 = jnp.float32
BF16 = jnp.bfloat16


def moe_kernel(nz, capacity, tok_hbm, ids_hbm, slots_hbm, gates_hbm, wg_hbm, wu_hbm, wd_hbm, out_ref,
               ids_ref, slots_ref, gates_ref, tok_all, meta_all, wg, wu, wd, pick, pick_t, slot_gate, buf, hid,
               acc, die_out, die_in, ring0, ring1, ring2, ring3,
               in_sem, route_sem, gate_sem, down_sem, ag_send, ag_recv, agm_send, agm_recv, die_send, die_recv,
               diem_send, diem_recv, sum_send, sum_recv, rs_send, rs_recv):
    rows = tok_hbm.shape[0]
    dim = tok_hbm.shape[1]
    n_exp, _, ffn = wg.shape
    n_col = dim // COLS
    half = rows // 2
    far = nz // 2
    side = nz * rows
    me = lax.axis_index('ep')
    z = me // CORES
    core = me % CORES
    right = {'ep': ((z + 1) % nz) * CORES + core}
    left = {'ep': ((z + nz - 1) % nz) * CORES + core}
    partner = {'ep': z * CORES + (1 - core)}
    nbr = (right, left)
    piece = dim // PIECES

    barrier = pltpu.get_barrier_semaphore()
    for dev in (right, left, partner):
        pl.semaphore_signal(barrier, inc=1, device_id=dev, device_id_type=MESH)
    own = pltpu.make_async_copy(tok_hbm, tok_all.at[0], in_sem)
    own.start()
    routes = [pltpu.make_async_copy(src, dst, route_sem.at[i]) for i, (src, dst) in enumerate(
        ((ids_hbm, ids_ref), (slots_hbm, slots_ref), (gates_hbm, gates_ref)))]
    for copy in routes:
        copy.start()

    def gate_copies(e):
        return (pltpu.make_async_copy(wg_hbm.at[e], wg.at[e], gate_sem.at[0]),
                pltpu.make_async_copy(wu_hbm.at[e], wu.at[e], gate_sem.at[1]))

    def down_copy(q):
        cols = pl.ds(pl.multiple_of(q * COLS, COLS), COLS)
        return pltpu.make_async_copy(wd_hbm.at[:, :, cols], wd.at[q], down_sem)

    for e in range(n_exp):
        for copy in gate_copies(e):
            copy.start(priority=1)
    for q in range(n_col):
        down_copy(q).start(priority=1)

    for copy in routes:
        copy.wait()
    meta_all[0] = jnp.concatenate(
        [ids_ref[...].astype(F32), slots_ref[...].astype(F32), gates_ref[...],
         jnp.zeros(gates_ref.shape, F32)], axis=1)
    pl.semaphore_wait(barrier, 3)
    own.wait()

    order = [0]
    for hop in range(1, far):
        order += [hop, nz - hop]
    order.append(far)
    place = {j: order.index(j) for j in range(nz)}
    quad = nz // 2

    def spot(other, j):
        return (place[j] // quad) * nz + other * quad + place[j] % quad

    def landed(ref, sem):
        pltpu.make_async_copy(ref, ref, sem).wait()

    def cols_of(p):
        return pl.ds(p * piece, piece)

    def ring_copy(way, hop, p):
        src = (nz - hop + 1) % nz if way == 0 else hop - 1
        dst = nz - hop if way == 0 else hop
        return pltpu.make_async_remote_copy(
            tok_all.at[spot(0, src), :, cols_of(p)], tok_all.at[spot(0, dst), :, cols_of(p)],
            ag_send, ag_recv.at[way, hop - 1, p], device_id=nbr[way], device_id_type=MESH)

    def ring_meta(way, hop):
        src = (nz - hop + 1) % nz if way == 0 else hop - 1
        dst = nz - hop if way == 0 else hop
        return pltpu.make_async_remote_copy(
            meta_all.at[spot(0, src)], meta_all.at[spot(0, dst)], agm_send, agm_recv.at[way, hop - 1],
            device_id=nbr[way], device_id_type=MESH)

    def die_copy(j, p):
        return pltpu.make_async_remote_copy(
            tok_all.at[spot(0, j), :, cols_of(p)], tok_all.at[spot(1, j), :, cols_of(p)],
            die_send, die_recv.at[place[j] // quad], device_id=partner, device_id_type=MESH)

    def die_meta(j):
        return pltpu.make_async_remote_copy(
            meta_all.at[spot(0, j)], meta_all.at[spot(1, j)], diem_send, diem_recv.at[place[j] // quad],
            device_id=partner, device_id_type=MESH)

    def on_ring(way, hop, p):
        if hop < far:
            return True
        return hop == far and (p < PIECES // 2) == (way == 0)

    def meta_on_ring(way, hop):
        return hop < far or (hop == far and way == 0)

    for way in range(2):
        ring_meta(way, 1).start()
    for p in range(PIECES):
        for way in range(2):
            if on_ring(way, 1, p):
                ring_copy(way, 1, p).start()
    die_meta(0).start()
    for p in range(PIECES):
        die_copy(0, p).start()

    def take_meta(hop):
        for way in range(2):
            if meta_on_ring(way, hop):
                ring_meta(way, hop).wait_recv()
                if meta_on_ring(way, hop + 1):
                    ring_meta(way, hop + 1).start()
                die_meta(nz - hop if way == 0 else hop).start()

    def take_tokens(hop, pieces=range(PIECES), fill=()):
        for p in pieces:
            for work in fill[p:p + 1]:
                work()
            for way in range(2):
                if on_ring(way, hop, p):
                    ring_copy(way, hop, p).wait_recv()
                    if on_ring(way, hop + 1, p):
                        ring_copy(way, hop + 1, p).start()
                    die_copy(nz - hop if way == 0 else hop, p).start()

    lane = lax.broadcasted_iota(jnp.int32, (8, 128), 1)
    per = 128 // rows
    slot_row = lax.broadcasted_iota(jnp.int32, (capacity, 128), 0).astype(F32) + 1.0
    slot_lane = lax.broadcasted_iota(jnp.int32, (128, capacity), 1).astype(F32) + 1.0

    def one_hots(g):
        ids = jnp.zeros((8, 128), F32)
        slots = jnp.zeros((8, 128), F32)
        gates = jnp.zeros((8, 128), F32)
        for i in range(per):
            tile = meta_all[g * per + i]
            here = (lane >= i * rows) & (lane < (i + 1) * rows)
            ids = jnp.where(here, pltpu.roll(tile, (i * rows) % 128, 1), ids)
            slots = jnp.where(here, pltpu.roll(tile, ((i - 1) * rows) % 128, 1), slots)
            gates = jnp.where(here, pltpu.roll(tile, ((i - 2) * rows) % 128, 1), gates)
        slot_rows = []
        for e in range(n_exp):
            mine = ids == (me * n_exp + e).astype(F32)
            slot_e = jnp.sum(jnp.where(mine, slots + 1.0, 0.0), axis=0, keepdims=True)
            gate_e = jnp.sum(jnp.where(mine, gates, 0.0), axis=0, keepdims=True)
            hit = slot_row == slot_e
            span = slice(e * capacity, (e + 1) * capacity)
            pick[span, g * 128:(g + 1) * 128] = jnp.where(hit, 1.0, 0.0).astype(BF16)
            gate_sum = jnp.broadcast_to(jnp.sum(jnp.where(hit, gate_e, 0.0), axis=1, keepdims=True), (capacity, 128))
            slot_gate[span, :] = gate_sum if g == 0 else slot_gate[span, :] + gate_sum
            slot_rows.append(slot_e)
        table = jnp.concatenate(slot_rows + [jnp.zeros((8 - n_exp, 128), F32)], axis=0).T
        base = ((g % 2) * 2 + g // 2) * 128
        for e in range(n_exp):
            pick_t[base:base + 128, e * capacity:(e + 1) * capacity] = jnp.where(
                slot_lane == table[:, e:e + 1], 1.0, 0.0).astype(BF16)

    def gather(part, blocks):
        for n in blocks:
            cols = slice(n * 512, (n + 1) * 512)
            block = tok_all[part * nz:(part + 1) * nz, :, cols].reshape(nz * rows, 512)
            got = jnp.dot(pick[:, part * nz * rows:(part + 1) * nz * rows], block, preferred_element_type=F32)
            if part == 0:
                buf[:, cols] = got.astype(BF16)
            else:
                buf[:, cols] = (buf[:, cols].astype(F32) + got).astype(BF16)

    def others(part):
        return slice(part * nz + quad, (part + 1) * nz)

    def near_routes():
        landed(meta_all.at[others(0)], diem_recv.at[0])

    def near_blocks():
        landed(tok_all.at[others(0)], die_recv.at[0])
        gather(0, (0,))

    wide = range(dim // 512)
    fills = {2: [lambda: None, near_routes, lambda: one_hots(0), lambda: one_hots(1)],
             3: [lambda: None, near_blocks] + [functools.partial(gather, 0, (n,)) for n in wide[1:3]]}
    for hop in range(1, far):
        take_meta(hop)
        take_tokens(hop, fill=fills.get(hop, ()))
    take_meta(far)
    gather(0, wide[3:])
    take_tokens(far, range(0, PIECES, 2))
    landed(meta_all.at[others(1)], diem_recv.at[1])
    one_hots(2)
    take_tokens(far, range(1, PIECES, 2))
    one_hots(3)
    landed(tok_all.at[others(1)], die_recv.at[1])
    landed(wg, gate_sem.at[0])
    landed(wu, gate_sem.at[1])
    landed(wd, down_sem)
    gather(1, wide)
    for e in range(n_exp):
        here = slice(e * capacity, (e + 1) * capacity)
        for n in range(ffn // 512):
            cols = slice(n * 512, (n + 1) * 512)
            x = buf[here, :]
            gate_h = jnp.dot(x, wg[e, :, cols], preferred_element_type=F32)
            up_h = jnp.dot(x, wu[e, :, cols], preferred_element_type=F32)
            hid[here, cols] = (jax.nn.silu(gate_h) * up_h).astype(BF16)

    split = (nz - 3) * rows

    def span_of(part):
        return slice(split, side) if part == 0 else slice(0, split)

    def sum_copy(q, part):
        span = span_of(part)
        return pltpu.make_async_remote_copy(
            die_out.at[q, span], die_in.at[q, span], sum_send, sum_recv.at[part, q],
            device_id=partner, device_id_type=MESH)

    def block_of(way, step):
        return far - step if way == 0 else (far + step) % nz

    def rs_copy(way, kind, q):
        first = slice(0, half) if way == 0 else slice(half, rows)
        second = slice(half, rows) if way == 0 else slice(0, half)
        step, part, dst = ((0, first, ring0), (1, second, ring1), (1, first, ring1),
                           (2, slice(0, rows), ring2), (3, slice(0, rows), ring3))[kind]
        base = place[block_of(way, step)] * rows
        src = acc.at[q, pl.ds(base + part.start, part.stop - part.start), :]
        if kind == 0:
            to = ring0.at[way, q]
        else:
            to = dst.at[way, q, pl.ds(part.start, part.stop - part.start), :]
        return pltpu.make_async_remote_copy(
            src, to, rs_send.at[step], rs_recv.at[step, q], device_id=nbr[way], device_id_type=MESH)

    def send_own(q):
        sum_copy(q, 0).wait_recv()
        acc[q, split:side, :] = acc[q, split:side, :] + die_in[q, split:side, :]
        for kind in (0, 1):
            for way in range(2):
                rs_copy(way, kind, q).start()

    def add_rest(q):
        sum_copy(q, 1).wait_recv()
        acc[q, 0:split, :] = acc[q, 0:split, :] + die_in[q, 0:split, :]

    rings = (ring0, ring1, ring2, ring3)

    def sums(q, step):
        landed(rings[step - 1].at[:, q], rs_recv.at[step - 1, q])
        for way in range(2):
            lo = place[block_of(way, step)] * rows
            size = rows
            if step == 1:
                lo, size = lo + (0 if way == 0 else half), half
            acc[q, lo:lo + size, :] = acc[q, lo:lo + size, :] + rings[step - 1][way, q]
            rs_copy(way, step + 1, q).start()

    slots = n_exp * capacity

    def project(q):
        for e in range(n_exp):
            span = slice(e * capacity, (e + 1) * capacity)
            res = jnp.dot(hid[span, :], wd[q, e], preferred_element_type=F32)
            res = res * jnp.concatenate([slot_gate[span, :]] * (COLS // 128), axis=1)
            hi = res.astype(BF16)
            rest = res - hi.astype(F32)
            mid = rest.astype(BF16)
            low = (rest - mid.astype(F32)).astype(BF16)
            for i, value in enumerate((hi, mid, low)):
                wg[q, i * slots + e * capacity:i * slots + (e + 1) * capacity, 0:COLS] = value

    def add_up(q, part):
        span = span_of(part)
        size = span.stop - span.start
        onehot = jnp.concatenate(
            [pick_t[span, :], pick_t[side + span.start:side + span.stop, :]], axis=0)
        total = jnp.dot(onehot, wg[q, 0:slots, 0:COLS], preferred_element_type=F32)
        for i in (1, 2):
            total = total + jnp.dot(onehot, wg[q, i * slots:(i + 1) * slots, 0:COLS], preferred_element_type=F32)
        acc[q, span, :] = total[0:size]
        die_out[q, span, :] = total[size:2 * size]

    project(0)
    for q in range(n_col):
        add_up(q, 0)
        if q + 1 < n_col:
            project(q + 1)
        sum_copy(q, 0).start()
        if q >= 1:
            send_own(q - 1)
    for q in range(n_col):
        add_up(q, 1)
        sum_copy(q, 1).start()
        if q == 0:
            send_own(n_col - 1)
        sums(q, 1)
    for step in (2, 3):
        for q in range(n_col):
            if step == 2:
                add_rest(q)
            sums(q, step)
    landed(tok_all.at[0:nz - 1], ag_send)
    landed(tok_all.at[0:nz], die_send)
    landed(meta_all.at[0:nz - 1], agm_send)
    landed(meta_all.at[0:nz], diem_send)
    landed(die_out, sum_send)
    for ring in range(3):
        landed(rings[ring], rs_send.at[ring])
    for q in range(n_col):
        landed(ring3.at[:, q], rs_recv.at[3, q])
        cols = slice(q * COLS, (q + 1) * COLS)
        out_ref[:, cols] = (acc[q, 0:rows, :] + (ring3[0, q] + ring3[1, q])).astype(out_ref.dtype)

    landed(ring3, rs_send.at[3])


def solution(mesh):
    row_spec = P(('dp', 'ep'), None)
    exp_spec = P('ep', None, None)
    devs = mesh.shape['ep']
    nz = devs // CORES

    def local_moe(tok_rows, expert_ids, gate_weights, slot_ids, w_gate, w_up, w_down):
        rows, dim = tok_rows.shape
        top_k = expert_ids.shape[1]
        n_exp, _, ffn = w_gate.shape
        capacity = 2 * top_k * rows // n_exp
        n_col = dim // COLS
        far = nz // 2
        slots = n_exp * capacity
        total = devs * rows
        dma = pltpu.SemaphoreType.DMA
        vmem = pltpu.VMEM
        scratch = [
            vmem((top_k, rows), jnp.int32), vmem((top_k, rows), jnp.int32), vmem((top_k, rows), F32),
            vmem((devs, rows, dim), BF16), vmem((devs, 8, 128), F32),
            vmem((n_exp, dim, ffn), BF16), vmem((n_exp, dim, ffn), BF16),
            vmem((n_col, n_exp, ffn, COLS), BF16),
            vmem((slots, total), BF16), vmem((total, slots), BF16), vmem((slots, 128), F32),
            vmem((slots, dim), BF16), vmem((slots, ffn), BF16),
            vmem((n_col, nz * rows, COLS), F32), vmem((n_col, nz * rows, COLS), F32), vmem((n_col, nz * rows, COLS), F32),
            vmem((2, n_col, rows // 2, COLS), F32),
            vmem((2, n_col, rows, COLS), F32), vmem((2, n_col, rows, COLS), F32), vmem((2, n_col, rows, COLS), F32),
            dma, dma((3,)), dma((2,)), dma,
            dma, dma((2, far, PIECES)), dma, dma((2, far)),
            dma, dma((2,)), dma, dma((2,)),
            dma, dma((2, n_col)), dma((4,)), dma((4, n_col)),
        ]
        anyspace = pl.BlockSpec(memory_space=pl.ANY)
        in_vmem = pl.BlockSpec(memory_space=pltpu.VMEM)
        flops = 6 * slots * dim * ffn
        return pl.pallas_call(
            functools.partial(moe_kernel, nz, capacity),
            out_shape=jax.ShapeDtypeStruct((rows, dim), tok_rows.dtype),
            in_specs=[anyspace] * 7,
            out_specs=in_vmem,
            scratch_shapes=scratch,
            name='routed_experts',
            cost_estimate=pl.CostEstimate(flops=flops, bytes_accessed=6 * n_exp * dim * ffn, transcendentals=slots * ffn),
            compiler_params=pltpu.CompilerParams(
                collective_id=0, has_side_effects=True, vmem_limit_bytes=67043328),
        )(tok_rows, expert_ids.T, slot_ids.T, gate_weights.T, w_gate, w_up, w_down)

    return jax.shard_map(local_moe, mesh=mesh, in_specs=(row_spec, row_spec, row_spec, row_spec, exp_spec, exp_spec, exp_spec), out_specs=row_spec, check_vma=False)
```

```python
import functools

import jax
import jax.numpy as jnp
from jax import lax
from jax.experimental import pallas as pl
from jax.experimental.pallas import tpu as pltpu
from jax.sharding import PartitionSpec as P

CORES = 2
PIECES = 4
COLS = 512
MESH = pl.DeviceIdType.MESH
F32 = jnp.float32
BF16 = jnp.bfloat16


def moe_kernel(nz, capacity, tok_hbm, ids_hbm, slots_hbm, gates_hbm, wg_hbm, wu_hbm, wd_hbm, out_ref,
               ids_ref, slots_ref, gates_ref, tok_all, meta_all, wg, wu, wd, pick, pick_t, slot_gate, buf, hid,
               acc, die_out, die_in, ring0, ring1, ring2, ring3,
               in_sem, route_sem, gate_sem, down_sem, ag_send, ag_recv, agm_send, agm_recv, die_send, die_recv,
               diem_send, diem_recv, sum_send, sum_recv, rs_send, rs_recv):
    rows = tok_hbm.shape[0]
    dim = tok_hbm.shape[1]
    n_exp, _, ffn = wg.shape
    n_col = dim // COLS
    half = rows // 2
    far = nz // 2
    side = nz * rows
    me = lax.axis_index('ep')
    z = me // CORES
    core = me % CORES
    right = {'ep': ((z + 1) % nz) * CORES + core}
    left = {'ep': ((z + nz - 1) % nz) * CORES + core}
    partner = {'ep': z * CORES + (1 - core)}
    nbr = (right, left)
    piece = dim // PIECES

    barrier = pltpu.get_barrier_semaphore()
    for dev in (right, left, partner):
        pl.semaphore_signal(barrier, inc=1, device_id=dev, device_id_type=MESH)
    own = pltpu.make_async_copy(tok_hbm, tok_all.at[0], in_sem)
    own.start()
    routes = [pltpu.make_async_copy(src, dst, route_sem.at[i]) for i, (src, dst) in enumerate(
        ((ids_hbm, ids_ref), (slots_hbm, slots_ref), (gates_hbm, gates_ref)))]
    for copy in routes:
        copy.start()

    def gate_copies(e):
        return (pltpu.make_async_copy(wg_hbm.at[e], wg.at[e], gate_sem.at[0]),
                pltpu.make_async_copy(wu_hbm.at[e], wu.at[e], gate_sem.at[1]))

    def down_copy(q):
        cols = pl.ds(pl.multiple_of(q * COLS, COLS), COLS)
        return pltpu.make_async_copy(wd_hbm.at[:, :, cols], wd.at[q], down_sem)

    for e in range(n_exp):
        for copy in gate_copies(e):
            copy.start(priority=1)
    for q in range(n_col):
        down_copy(q).start(priority=1)

    for copy in routes:
        copy.wait()
    meta_all[0] = jnp.concatenate(
        [ids_ref[...].astype(F32), slots_ref[...].astype(F32), gates_ref[...],
         jnp.zeros(gates_ref.shape, F32)], axis=1)
    pl.semaphore_wait(barrier, 3)
    own.wait()

    order = [0]
    for hop in range(1, far):
        order += [hop, nz - hop]
    order.append(far)
    place = {j: order.index(j) for j in range(nz)}
    quad = nz // 2

    def spot(other, j):
        return (place[j] // quad) * nz + other * quad + place[j] % quad

    def landed(ref, sem):
        pltpu.make_async_copy(ref, ref, sem).wait()

    def cols_of(p):
        return pl.ds(p * piece, piece)

    def ring_copy(way, hop, p):
        src = (nz - hop + 1) % nz if way == 0 else hop - 1
        dst = nz - hop if way == 0 else hop
        return pltpu.make_async_remote_copy(
            tok_all.at[spot(0, src), :, cols_of(p)], tok_all.at[spot(0, dst), :, cols_of(p)],
            ag_send, ag_recv.at[way, hop - 1, p], device_id=nbr[way], device_id_type=MESH)

    def ring_meta(way, hop):
        src = (nz - hop + 1) % nz if way == 0 else hop - 1
        dst = nz - hop if way == 0 else hop
        return pltpu.make_async_remote_copy(
            meta_all.at[spot(0, src)], meta_all.at[spot(0, dst)], agm_send, agm_recv.at[way, hop - 1],
            device_id=nbr[way], device_id_type=MESH)

    def die_copy(j, p):
        return pltpu.make_async_remote_copy(
            tok_all.at[spot(0, j), :, cols_of(p)], tok_all.at[spot(1, j), :, cols_of(p)],
            die_send, die_recv.at[place[j] // quad], device_id=partner, device_id_type=MESH)

    def die_meta(j):
        return pltpu.make_async_remote_copy(
            meta_all.at[spot(0, j)], meta_all.at[spot(1, j)], diem_send, diem_recv.at[place[j] // quad],
            device_id=partner, device_id_type=MESH)

    def on_ring(way, hop, p):
        if hop < far:
            return True
        return hop == far and (p < PIECES // 2) == (way == 0)

    def meta_on_ring(way, hop):
        return hop < far or (hop == far and way == 0)

    for p in range(PIECES):
        for way in range(2):
            if on_ring(way, 1, p):
                ring_copy(way, 1, p).start()
            if p == 0:
                ring_meta(way, 1).start()
    die_meta(0).start()
    for p in range(PIECES):
        die_copy(0, p).start()

    def take_meta(hop):
        for way in range(2):
            if meta_on_ring(way, hop):
                ring_meta(way, hop).wait_recv()
                if meta_on_ring(way, hop + 1):
                    ring_meta(way, hop + 1).start()
                die_meta(nz - hop if way == 0 else hop).start()

    def take_tokens(hop, pieces=range(PIECES), fill=()):
        for p in pieces:
            for work in fill[p:p + 1]:
                work()
            for way in range(2):
                if on_ring(way, hop, p):
                    ring_copy(way, hop, p).wait_recv()
                    if on_ring(way, hop + 1, p):
                        ring_copy(way, hop + 1, p).start()
                    die_copy(nz - hop if way == 0 else hop, p).start()

    lane = lax.broadcasted_iota(jnp.int32, (8, 128), 1)
    per = 128 // rows
    slot_row = lax.broadcasted_iota(jnp.int32, (capacity, 128), 0).astype(F32) + 1.0
    slot_lane = lax.broadcasted_iota(jnp.int32, (128, capacity), 1).astype(F32) + 1.0

    def one_hots(g):
        ids = jnp.zeros((8, 128), F32)
        slots = jnp.zeros((8, 128), F32)
        gates = jnp.zeros((8, 128), F32)
        for i in range(per):
            tile = meta_all[g * per + i]
            here = (lane >= i * rows) & (lane < (i + 1) * rows)
            ids = jnp.where(here, pltpu.roll(tile, (i * rows) % 128, 1), ids)
            slots = jnp.where(here, pltpu.roll(tile, ((i - 1) * rows) % 128, 1), slots)
            gates = jnp.where(here, pltpu.roll(tile, ((i - 2) * rows) % 128, 1), gates)
        slot_rows = []
        for e in range(n_exp):
            mine = ids == (me * n_exp + e).astype(F32)
            slot_e = jnp.sum(jnp.where(mine, slots + 1.0, 0.0), axis=0, keepdims=True)
            gate_e = jnp.sum(jnp.where(mine, gates, 0.0), axis=0, keepdims=True)
            hit = slot_row == slot_e
            span = slice(e * capacity, (e + 1) * capacity)
            pick[span, g * 128:(g + 1) * 128] = jnp.where(hit, 1.0, 0.0).astype(BF16)
            gate_sum = jnp.broadcast_to(jnp.sum(jnp.where(hit, gate_e, 0.0), axis=1, keepdims=True), (capacity, 128))
            slot_gate[span, :] = gate_sum if g == 0 else slot_gate[span, :] + gate_sum
            slot_rows.append(slot_e)
        table = jnp.concatenate(slot_rows + [jnp.zeros((8 - n_exp, 128), F32)], axis=0).T
        base = ((g % 2) * 2 + g // 2) * 128
        for e in range(n_exp):
            pick_t[base:base + 128, e * capacity:(e + 1) * capacity] = jnp.where(
                slot_lane == table[:, e:e + 1], 1.0, 0.0).astype(BF16)

    def gather(part, blocks):
        for n in blocks:
            cols = slice(n * 512, (n + 1) * 512)
            block = tok_all[part * nz:(part + 1) * nz, :, cols].reshape(nz * rows, 512)
            got = jnp.dot(pick[:, part * nz * rows:(part + 1) * nz * rows], block, preferred_element_type=F32)
            if part == 0:
                buf[:, cols] = got.astype(BF16)
            else:
                buf[:, cols] = (buf[:, cols].astype(F32) + got).astype(BF16)

    def others(part):
        return slice(part * nz + quad, (part + 1) * nz)

    def near_routes():
        landed(meta_all.at[others(0)], diem_recv.at[0])

    def near_blocks():
        landed(tok_all.at[others(0)], die_recv.at[0])
        gather(0, (0,))

    wide = range(dim // 512)
    fills = {2: [lambda: None, near_routes, lambda: one_hots(0), lambda: one_hots(1)],
             3: [lambda: None, near_blocks] + [functools.partial(gather, 0, (n,)) for n in wide[1:3]]}
    for hop in range(1, far):
        take_meta(hop)
        take_tokens(hop, fill=fills.get(hop, ()))
    take_meta(far)
    take_tokens(far, range(0, PIECES, 2))
    take_tokens(far, range(1, PIECES, 2))
    landed(meta_all.at[others(1)], diem_recv.at[1])
    one_hots(2)
    one_hots(3)
    gather(0, wide[3:])
    landed(tok_all.at[others(1)], die_recv.at[1])
    landed(wg, gate_sem.at[0])
    landed(wu, gate_sem.at[1])
    landed(wd, down_sem)
    gather(1, wide)
    for e in range(n_exp):
        here = slice(e * capacity, (e + 1) * capacity)
        for n in range(ffn // 512):
            cols = slice(n * 512, (n + 1) * 512)
            x = buf[here, :]
            gate_h = jnp.dot(x, wg[e, :, cols], preferred_element_type=F32)
            up_h = jnp.dot(x, wu[e, :, cols], preferred_element_type=F32)
            hid[here, cols] = (jax.nn.silu(gate_h) * up_h).astype(BF16)

    split = (nz - 3) * rows

    def span_of(part):
        return slice(split, side) if part == 0 else slice(0, split)

    def sum_copy(q, part):
        span = span_of(part)
        return pltpu.make_async_remote_copy(
            die_out.at[q, span], die_in.at[q, span], sum_send, sum_recv.at[part, q],
            device_id=partner, device_id_type=MESH)

    def block_of(way, step):
        return far - step if way == 0 else (far + step) % nz

    def rs_copy(way, kind, q):
        first = slice(0, half) if way == 0 else slice(half, rows)
        second = slice(half, rows) if way == 0 else slice(0, half)
        step, part, dst = ((0, first, ring0), (1, second, ring1), (1, first, ring1),
                           (2, slice(0, rows), ring2), (3, slice(0, rows), ring3))[kind]
        base = place[block_of(way, step)] * rows
        src = acc.at[q, pl.ds(base + part.start, part.stop - part.start), :]
        if kind == 0:
            to = ring0.at[way, q]
        else:
            to = dst.at[way, q, pl.ds(part.start, part.stop - part.start), :]
        return pltpu.make_async_remote_copy(
            src, to, rs_send.at[step], rs_recv.at[step, q], device_id=nbr[way], device_id_type=MESH)

    def send_own(q):
        sum_copy(q, 0).wait_recv()
        acc[q, split:side, :] = acc[q, split:side, :] + die_in[q, split:side, :]
        for kind in (0, 1):
            for way in range(2):
                rs_copy(way, kind, q).start()

    def add_rest(q):
        sum_copy(q, 1).wait_recv()
        acc[q, 0:split, :] = acc[q, 0:split, :] + die_in[q, 0:split, :]

    rings = (ring0, ring1, ring2, ring3)

    def sums(q, step):
        landed(rings[step - 1].at[:, q], rs_recv.at[step - 1, q])
        for way in range(2):
            lo = place[block_of(way, step)] * rows
            size = rows
            if step == 1:
                lo, size = lo + (0 if way == 0 else half), half
            acc[q, lo:lo + size, :] = acc[q, lo:lo + size, :] + rings[step - 1][way, q]
            rs_copy(way, step + 1, q).start()

    slots = n_exp * capacity

    def project(q):
        for e in range(n_exp):
            span = slice(e * capacity, (e + 1) * capacity)
            res = jnp.dot(hid[span, :], wd[q, e], preferred_element_type=F32)
            res = res * jnp.concatenate([slot_gate[span, :]] * (COLS // 128), axis=1)
            hi = res.astype(BF16)
            rest = res - hi.astype(F32)
            mid = rest.astype(BF16)
            low = (rest - mid.astype(F32)).astype(BF16)
            for i, value in enumerate((hi, mid, low)):
                wg[q, i * slots + e * capacity:i * slots + (e + 1) * capacity, 0:COLS] = value

    def add_up(q, part):
        span = span_of(part)
        size = span.stop - span.start
        onehot = jnp.concatenate(
            [pick_t[span, :], pick_t[side + span.start:side + span.stop, :]], axis=0)
        total = jnp.dot(onehot, wg[q, 0:slots, 0:COLS], preferred_element_type=F32)
        for i in (1, 2):
            total = total + jnp.dot(onehot, wg[q, i * slots:(i + 1) * slots, 0:COLS], preferred_element_type=F32)
        acc[q, span, :] = total[0:size]
        die_out[q, span, :] = total[size:2 * size]

    project(0)
    for q in range(n_col):
        add_up(q, 0)
        if q + 1 < n_col:
            project(q + 1)
        sum_copy(q, 0).start()
        if q >= 1:
            send_own(q - 1)
    for q in range(n_col):
        add_up(q, 1)
        sum_copy(q, 1).start()
        if q == 0:
            send_own(n_col - 1)
        else:
            add_rest(q - 1)
        sums(q, 1)
    for step in (2, 3):
        for q in range(n_col):
            sums(q, step)
            if step == 2 and q == 0:
                add_rest(n_col - 1)
    landed(tok_all.at[0:nz - 1], ag_send)
    landed(tok_all.at[0:nz], die_send)
    landed(meta_all.at[0:nz - 1], agm_send)
    landed(meta_all.at[0:nz], diem_send)
    landed(die_out, sum_send)
    for ring in range(3):
        landed(rings[ring], rs_send.at[ring])
    for q in range(n_col):
        landed(ring3.at[:, q], rs_recv.at[3, q])
        cols = slice(q * COLS, (q + 1) * COLS)
        out_ref[:, cols] = (acc[q, 0:rows, :] + (ring3[0, q] + ring3[1, q])).astype(out_ref.dtype)

    landed(ring3, rs_send.at[3])


def solution(mesh):
    row_spec = P(('dp', 'ep'), None)
    exp_spec = P('ep', None, None)
    devs = mesh.shape['ep']
    nz = devs // CORES

    def local_moe(tok_rows, expert_ids, gate_weights, slot_ids, w_gate, w_up, w_down):
        rows, dim = tok_rows.shape
        top_k = expert_ids.shape[1]
        n_exp, _, ffn = w_gate.shape
        capacity = 2 * top_k * rows // n_exp
        n_col = dim // COLS
        far = nz // 2
        slots = n_exp * capacity
        total = devs * rows
        dma = pltpu.SemaphoreType.DMA
        vmem = pltpu.VMEM
        scratch = [
            vmem((top_k, rows), jnp.int32), vmem((top_k, rows), jnp.int32), vmem((top_k, rows), F32),
            vmem((devs, rows, dim), BF16), vmem((devs, 8, 128), F32),
            vmem((n_exp, dim, ffn), BF16), vmem((n_exp, dim, ffn), BF16),
            vmem((n_col, n_exp, ffn, COLS), BF16),
            vmem((slots, total), BF16), vmem((total, slots), BF16), vmem((slots, 128), F32),
            vmem((slots, dim), BF16), vmem((slots, ffn), BF16),
            vmem((n_col, nz * rows, COLS), F32), vmem((n_col, nz * rows, COLS), F32), vmem((n_col, nz * rows, COLS), F32),
            vmem((2, n_col, rows // 2, COLS), F32),
            vmem((2, n_col, rows, COLS), F32), vmem((2, n_col, rows, COLS), F32), vmem((2, n_col, rows, COLS), F32),
            dma, dma((3,)), dma((2,)), dma,
            dma, dma((2, far, PIECES)), dma, dma((2, far)),
            dma, dma((2,)), dma, dma((2,)),
            dma, dma((2, n_col)), dma((4,)), dma((4, n_col)),
        ]
        anyspace = pl.BlockSpec(memory_space=pl.ANY)
        in_vmem = pl.BlockSpec(memory_space=pltpu.VMEM)
        flops = 6 * slots * dim * ffn
        return pl.pallas_call(
            functools.partial(moe_kernel, nz, capacity),
            out_shape=jax.ShapeDtypeStruct((rows, dim), tok_rows.dtype),
            in_specs=[anyspace] * 7,
            out_specs=in_vmem,
            scratch_shapes=scratch,
            name='routed_experts',
            cost_estimate=pl.CostEstimate(flops=flops, bytes_accessed=6 * n_exp * dim * ffn, transcendentals=slots * ffn),
            compiler_params=pltpu.CompilerParams(
                collective_id=0, has_side_effects=True, vmem_limit_bytes=67043328),
        )(tok_rows, expert_ids.T, slot_ids.T, gate_weights.T, w_gate, w_up, w_down)

    return jax.shard_map(local_moe, mesh=mesh, in_specs=(row_spec, row_spec, row_spec, row_spec, exp_spec, exp_spec, exp_spec), out_specs=row_spec, check_vma=False)
```

```python
import functools

import jax
import jax.numpy as jnp
from jax import lax
from jax.experimental import pallas as pl
from jax.experimental.pallas import tpu as pltpu
from jax.sharding import PartitionSpec as P

CORES = 2
PIECES = 4
COLS = 512
MESH = pl.DeviceIdType.MESH
F32 = jnp.float32
BF16 = jnp.bfloat16


def moe_kernel(nz, capacity, tok_hbm, ids_hbm, slots_hbm, gates_hbm, wg_hbm, wu_hbm, wd_hbm, out_ref,
               ids_ref, slots_ref, gates_ref, tok_all, meta_all, wg, wu, wd, pick, pick_t, slot_gate, buf, hid,
               acc, die_out, die_in, ring0, ring1, ring2, ring3,
               in_sem, route_sem, gate_sem, down_sem, ag_send, ag_recv, agm_send, agm_recv, die_send, die_recv,
               diem_send, diem_recv, sum_send, sum_recv, rs_send, rs_recv):
    rows = tok_hbm.shape[0]
    dim = tok_hbm.shape[1]
    n_exp, _, ffn = wg.shape
    n_col = dim // COLS
    half = rows // 2
    far = nz // 2
    side = nz * rows
    me = lax.axis_index('ep')
    z = me // CORES
    core = me % CORES
    right = {'ep': ((z + 1) % nz) * CORES + core}
    left = {'ep': ((z + nz - 1) % nz) * CORES + core}
    partner = {'ep': z * CORES + (1 - core)}
    nbr = (right, left)
    piece = dim // PIECES

    barrier = pltpu.get_barrier_semaphore()
    for dev in (right, left, partner):
        pl.semaphore_signal(barrier, inc=1, device_id=dev, device_id_type=MESH)
    own = pltpu.make_async_copy(tok_hbm, tok_all.at[0], in_sem)
    own.start()
    routes = [pltpu.make_async_copy(src, dst, route_sem.at[i]) for i, (src, dst) in enumerate(
        ((ids_hbm, ids_ref), (slots_hbm, slots_ref), (gates_hbm, gates_ref)))]
    for copy in routes:
        copy.start()

    def gate_copies(e):
        return (pltpu.make_async_copy(wg_hbm.at[e], wg.at[e], gate_sem.at[0]),
                pltpu.make_async_copy(wu_hbm.at[e], wu.at[e], gate_sem.at[1]))

    def down_copy(q):
        cols = pl.ds(pl.multiple_of(q * COLS, COLS), COLS)
        return pltpu.make_async_copy(wd_hbm.at[:, :, cols], wd.at[q], down_sem)

    for e in range(n_exp):
        for copy in gate_copies(e):
            copy.start(priority=1)
    for q in range(n_col):
        down_copy(q).start(priority=1)

    for copy in routes:
        copy.wait()
    meta_all[0] = jnp.concatenate(
        [ids_ref[...].astype(F32), slots_ref[...].astype(F32), gates_ref[...],
         jnp.zeros(gates_ref.shape, F32)], axis=1)
    pl.semaphore_wait(barrier, 3)
    own.wait()

    order = [0]
    for hop in range(1, far):
        order += [hop, nz - hop]
    order.append(far)
    place = {j: order.index(j) for j in range(nz)}
    quad = nz // 2

    def spot(other, j):
        return (place[j] // quad) * nz + other * quad + place[j] % quad

    def landed(ref, sem):
        pltpu.make_async_copy(ref, ref, sem).wait()

    def cols_of(p):
        return pl.ds(p * piece, piece)

    def ring_copy(way, hop, p):
        src = (nz - hop + 1) % nz if way == 0 else hop - 1
        dst = nz - hop if way == 0 else hop
        return pltpu.make_async_remote_copy(
            tok_all.at[spot(0, src), :, cols_of(p)], tok_all.at[spot(0, dst), :, cols_of(p)],
            ag_send, ag_recv.at[way, hop - 1, p], device_id=nbr[way], device_id_type=MESH)

    def ring_meta(way, hop):
        src = (nz - hop + 1) % nz if way == 0 else hop - 1
        dst = nz - hop if way == 0 else hop
        return pltpu.make_async_remote_copy(
            meta_all.at[spot(0, src)], meta_all.at[spot(0, dst)], agm_send, agm_recv.at[way, hop - 1],
            device_id=nbr[way], device_id_type=MESH)

    def die_copy(j, p):
        return pltpu.make_async_remote_copy(
            tok_all.at[spot(0, j), :, cols_of(p)], tok_all.at[spot(1, j), :, cols_of(p)],
            die_send, die_recv.at[place[j] // quad], device_id=partner, device_id_type=MESH)

    def die_meta(j):
        return pltpu.make_async_remote_copy(
            meta_all.at[spot(0, j)], meta_all.at[spot(1, j)], diem_send, diem_recv.at[place[j] // quad],
            device_id=partner, device_id_type=MESH)

    def on_ring(way, hop, p):
        if hop < far:
            return True
        return hop == far and (p < PIECES // 2) == (way == 0)

    def meta_on_ring(way, hop):
        return hop < far or (hop == far and way == 0)

    for way in range(2):
        ring_meta(way, 1).start()
    for p in range(PIECES):
        for way in range(2):
            if on_ring(way, 1, p):
                ring_copy(way, 1, p).start()
    die_meta(0).start()
    for p in range(PIECES):
        die_copy(0, p).start()

    def take_meta(hop):
        for way in range(2):
            if meta_on_ring(way, hop):
                ring_meta(way, hop).wait_recv()
                if meta_on_ring(way, hop + 1):
                    ring_meta(way, hop + 1).start()
                die_meta(nz - hop if way == 0 else hop).start()

    def take_tokens(hop, pieces=range(PIECES), fill=()):
        for p in pieces:
            for work in fill[p:p + 1]:
                work()
            for way in range(2):
                if on_ring(way, hop, p):
                    ring_copy(way, hop, p).wait_recv()
                    if on_ring(way, hop + 1, p):
                        ring_copy(way, hop + 1, p).start()
                    die_copy(nz - hop if way == 0 else hop, p).start()

    lane = lax.broadcasted_iota(jnp.int32, (8, 128), 1)
    per = 128 // rows
    slot_row = lax.broadcasted_iota(jnp.int32, (capacity, 128), 0).astype(F32) + 1.0
    slot_lane = lax.broadcasted_iota(jnp.int32, (128, capacity), 1).astype(F32) + 1.0

    def one_hots(g):
        ids = jnp.zeros((8, 128), F32)
        slots = jnp.zeros((8, 128), F32)
        gates = jnp.zeros((8, 128), F32)
        for i in range(per):
            tile = meta_all[g * per + i]
            here = (lane >= i * rows) & (lane < (i + 1) * rows)
            ids = jnp.where(here, pltpu.roll(tile, (i * rows) % 128, 1), ids)
            slots = jnp.where(here, pltpu.roll(tile, ((i - 1) * rows) % 128, 1), slots)
            gates = jnp.where(here, pltpu.roll(tile, ((i - 2) * rows) % 128, 1), gates)
        slot_rows = []
        for e in range(n_exp):
            mine = ids == (me * n_exp + e).astype(F32)
            slot_e = jnp.sum(jnp.where(mine, slots + 1.0, 0.0), axis=0, keepdims=True)
            gate_e = jnp.sum(jnp.where(mine, gates, 0.0), axis=0, keepdims=True)
            hit = slot_row == slot_e
            span = slice(e * capacity, (e + 1) * capacity)
            pick[span, g * 128:(g + 1) * 128] = jnp.where(hit, 1.0, 0.0).astype(BF16)
            gate_sum = jnp.broadcast_to(jnp.sum(jnp.where(hit, gate_e, 0.0), axis=1, keepdims=True), (capacity, 128))
            slot_gate[span, :] = gate_sum if g == 0 else slot_gate[span, :] + gate_sum
            slot_rows.append(slot_e)
        table = jnp.concatenate(slot_rows + [jnp.zeros((8 - n_exp, 128), F32)], axis=0).T
        base = ((g % 2) * 2 + g // 2) * 128
        for e in range(n_exp):
            pick_t[base:base + 128, e * capacity:(e + 1) * capacity] = jnp.where(
                slot_lane == table[:, e:e + 1], 1.0, 0.0).astype(BF16)

    def gather(part, blocks):
        for n in blocks:
            cols = slice(n * 512, (n + 1) * 512)
            block = tok_all[part * nz:(part + 1) * nz, :, cols].reshape(nz * rows, 512)
            got = jnp.dot(pick[:, part * nz * rows:(part + 1) * nz * rows], block, preferred_element_type=F32)
            if part == 0:
                buf[:, cols] = got.astype(BF16)
            else:
                buf[:, cols] = (buf[:, cols].astype(F32) + got).astype(BF16)

    def others(part):
        return slice(part * nz + quad, (part + 1) * nz)

    def near_routes():
        landed(meta_all.at[others(0)], diem_recv.at[0])

    def near_blocks():
        landed(tok_all.at[others(0)], die_recv.at[0])
        gather(0, (0,))

    wide = range(dim // 512)
    fills = {2: [lambda: None, near_routes, lambda: one_hots(0), lambda: one_hots(1)],
             3: [lambda: None, near_blocks] + [functools.partial(gather, 0, (n,)) for n in wide[1:3]]}
    for hop in range(1, far):
        take_meta(hop)
        take_tokens(hop, fill=fills.get(hop, ()))
    take_meta(far)
    take_tokens(far, range(0, PIECES, 2))
    take_tokens(far, range(1, PIECES, 2))
    landed(meta_all.at[others(1)], diem_recv.at[1])
    one_hots(2)
    one_hots(3)
    gather(0, wide[3:])
    landed(tok_all.at[others(1)], die_recv.at[1])
    landed(wg, gate_sem.at[0])
    landed(wu, gate_sem.at[1])
    landed(wd, down_sem)
    gather(1, wide)
    for e in range(n_exp):
        here = slice(e * capacity, (e + 1) * capacity)
        for n in range(ffn // 512):
            cols = slice(n * 512, (n + 1) * 512)
            x = buf[here, :]
            gate_h = jnp.dot(x, wg[e, :, cols], preferred_element_type=F32)
            up_h = jnp.dot(x, wu[e, :, cols], preferred_element_type=F32)
            hid[here, cols] = (jax.nn.silu(gate_h) * up_h).astype(BF16)

    split = (nz - 3) * rows

    def span_of(part):
        return slice(split, side) if part == 0 else slice(0, split)

    def sum_copy(q, part):
        span = span_of(part)
        return pltpu.make_async_remote_copy(
            die_out.at[q, span], die_in.at[q, span], sum_send, sum_recv.at[part, q],
            device_id=partner, device_id_type=MESH)

    def block_of(way, step):
        return far - step if way == 0 else (far + step) % nz

    def rs_copy(way, kind, q):
        first = slice(0, half) if way == 0 else slice(half, rows)
        second = slice(half, rows) if way == 0 else slice(0, half)
        step, part, dst = ((0, first, ring0), (1, second, ring1), (1, first, ring1),
                           (2, slice(0, rows), ring2), (3, slice(0, rows), ring3))[kind]
        base = place[block_of(way, step)] * rows
        src = acc.at[q, pl.ds(base + part.start, part.stop - part.start), :]
        if kind == 0:
            to = ring0.at[way, q]
        else:
            to = dst.at[way, q, pl.ds(part.start, part.stop - part.start), :]
        return pltpu.make_async_remote_copy(
            src, to, rs_send.at[step], rs_recv.at[step, q], device_id=nbr[way], device_id_type=MESH)

    def send_own(q):
        sum_copy(q, 0).wait_recv()
        acc[q, split:side, :] = acc[q, split:side, :] + die_in[q, split:side, :]
        for kind in (0, 1):
            for way in range(2):
                rs_copy(way, kind, q).start()

    def add_rest(q):
        sum_copy(q, 1).wait_recv()
        acc[q, 0:split, :] = acc[q, 0:split, :] + die_in[q, 0:split, :]

    rings = (ring0, ring1, ring2, ring3)

    def sums(q, step):
        landed(rings[step - 1].at[:, q], rs_recv.at[step - 1, q])
        for way in range(2):
            lo = place[block_of(way, step)] * rows
            size = rows
            if step == 1:
                lo, size = lo + (0 if way == 0 else half), half
            acc[q, lo:lo + size, :] = acc[q, lo:lo + size, :] + rings[step - 1][way, q]
            rs_copy(way, step + 1, q).start()

    slots = n_exp * capacity

    def project(q):
        for e in range(n_exp):
            span = slice(e * capacity, (e + 1) * capacity)
            res = jnp.dot(hid[span, :], wd[q, e], preferred_element_type=F32)
            res = res * jnp.concatenate([slot_gate[span, :]] * (COLS // 128), axis=1)
            hi = res.astype(BF16)
            rest = res - hi.astype(F32)
            mid = rest.astype(BF16)
            low = (rest - mid.astype(F32)).astype(BF16)
            for i, value in enumerate((hi, mid, low)):
                wg[q, i * slots + e * capacity:i * slots + (e + 1) * capacity, 0:COLS] = value

    def add_up(q, part):
        span = span_of(part)
        size = span.stop - span.start
        onehot = jnp.concatenate(
            [pick_t[span, :], pick_t[side + span.start:side + span.stop, :]], axis=0)
        total = jnp.dot(onehot, wg[q, 0:slots, 0:COLS], preferred_element_type=F32)
        for i in (1, 2):
            total = total + jnp.dot(onehot, wg[q, i * slots:(i + 1) * slots, 0:COLS], preferred_element_type=F32)
        acc[q, span, :] = total[0:size]
        die_out[q, span, :] = total[size:2 * size]

    project(0)
    for q in range(n_col):
        add_up(q, 0)
        if q + 1 < n_col:
            project(q + 1)
        sum_copy(q, 0).start()
        if q >= 1:
            send_own(q - 1)
    for q in range(n_col):
        add_up(q, 1)
        sum_copy(q, 1).start()
        if q == 0:
            send_own(n_col - 1)
        sums(q, 1)
    for step in (2, 3):
        for q in range(n_col):
            if step == 2:
                add_rest(q)
            sums(q, step)
    landed(tok_all.at[0:nz - 1], ag_send)
    landed(tok_all.at[0:nz], die_send)
    landed(meta_all.at[0:nz - 1], agm_send)
    landed(meta_all.at[0:nz], diem_send)
    landed(die_out, sum_send)
    for ring in range(3):
        landed(rings[ring], rs_send.at[ring])
    for q in range(n_col):
        landed(ring3.at[:, q], rs_recv.at[3, q])
        cols = slice(q * COLS, (q + 1) * COLS)
        out_ref[:, cols] = (acc[q, 0:rows, :] + (ring3[0, q] + ring3[1, q])).astype(out_ref.dtype)

    landed(ring3, rs_send.at[3])


def solution(mesh):
    row_spec = P(('dp', 'ep'), None)
    exp_spec = P('ep', None, None)
    devs = mesh.shape['ep']
    nz = devs // CORES

    def local_moe(tok_rows, expert_ids, gate_weights, slot_ids, w_gate, w_up, w_down):
        rows, dim = tok_rows.shape
        top_k = expert_ids.shape[1]
        n_exp, _, ffn = w_gate.shape
        capacity = 2 * top_k * rows // n_exp
        n_col = dim // COLS
        far = nz // 2
        slots = n_exp * capacity
        total = devs * rows
        dma = pltpu.SemaphoreType.DMA
        vmem = pltpu.VMEM
        scratch = [
            vmem((top_k, rows), jnp.int32), vmem((top_k, rows), jnp.int32), vmem((top_k, rows), F32),
            vmem((devs, rows, dim), BF16), vmem((devs, 8, 128), F32),
            vmem((n_exp, dim, ffn), BF16), vmem((n_exp, dim, ffn), BF16),
            vmem((n_col, n_exp, ffn, COLS), BF16),
            vmem((slots, total), BF16), vmem((total, slots), BF16), vmem((slots, 128), F32),
            vmem((slots, dim), BF16), vmem((slots, ffn), BF16),
            vmem((n_col, nz * rows, COLS), F32), vmem((n_col, nz * rows, COLS), F32), vmem((n_col, nz * rows, COLS), F32),
            vmem((2, n_col, rows // 2, COLS), F32),
            vmem((2, n_col, rows, COLS), F32), vmem((2, n_col, rows, COLS), F32), vmem((2, n_col, rows, COLS), F32),
            dma, dma((3,)), dma((2,)), dma,
            dma, dma((2, far, PIECES)), dma, dma((2, far)),
            dma, dma((2,)), dma, dma((2,)),
            dma, dma((2, n_col)), dma((4,)), dma((4, n_col)),
        ]
        anyspace = pl.BlockSpec(memory_space=pl.ANY)
        in_vmem = pl.BlockSpec(memory_space=pltpu.VMEM)
        flops = 6 * slots * dim * ffn
        return pl.pallas_call(
            functools.partial(moe_kernel, nz, capacity),
            out_shape=jax.ShapeDtypeStruct((rows, dim), tok_rows.dtype),
            in_specs=[anyspace] * 7,
            out_specs=in_vmem,
            scratch_shapes=scratch,
            name='routed_experts',
            cost_estimate=pl.CostEstimate(flops=flops, bytes_accessed=6 * n_exp * dim * ffn, transcendentals=slots * ffn),
            compiler_params=pltpu.CompilerParams(
                collective_id=0, has_side_effects=True, vmem_limit_bytes=67043328),
        )(tok_rows, expert_ids.T, slot_ids.T, gate_weights.T, w_gate, w_up, w_down)

    return jax.shard_map(local_moe, mesh=mesh, in_specs=(row_spec, row_spec, row_spec, row_spec, exp_spec, exp_spec, exp_spec), out_specs=row_spec, check_vma=False)
```
